128 devices in a mesh: dp: 32 (over y, x, core), leaf: 4 (over z).
Axes of the slice: x: 4, y: 4, z: 4, core: 2. Of those that a mesh axis runs over, the one named last changes fastest.
Arguments:
- predict: float32 [100, 1048576], P(None, ('dp', 'leaf')), may hold values from -6 to 256
- labels: int32 [1048576], P(('dp', 'leaf')), may hold values from 0 to 99
- leaf_ids: int32 [32, 1048576], P(None, ('dp', 'leaf')), may hold values from 0 to 63
Outputs:
- new_predict: float32 [100, 1048576], P(None, ('dp', 'leaf'))
- leaf_values: float32 [100, 2048], P(None, 'leaf')
The draws below stay inside these ranges and needn't reach their ends.
All inputs are finite; a program needn't handle non-finite values.
Results may differ from the reference program's by a relative error of at most 0.0044.
Values sent between devices are 32-bit elements; how exact they have to be, the bound alone decides.
A program may use at most 64 MiB of HBM per device.

```python
import jax
import jax.numpy as jnp
from jax import lax

CLASSES = 100
LEAVES = 64
TREES = 32
ROWS = 1048576


def draw_predict(key, part):
    base_key = jax.random.fold_in(key, 0)
    return 1.5 * jax.random.truncated_normal(base_key, -4.0, 4.0, (CLASSES, ROWS), jnp.float32)


def place_ends(values, rng, least, top_value):
    extent = values.shape
    spot = [jax.random.randint(jax.random.fold_in(rng, axis), (), 0, extent[axis]) for axis in range(len(extent))]
    values = values.at[tuple(spot)].set(least)
    longest = extent.index(max(extent))
    spot[longest] = (spot[longest] + 1) % extent[longest]
    return values.at[tuple(spot)].set(top_value)


def setup_inputs(seed: int = 0) -> dict:
    arg_keys = jax.random.split(jax.random.key(seed), 4)
    return {
        "predict": draw_predict(jax.random.fold_in(arg_keys[3], 71), 0),
        "labels": place_ends(jax.random.randint(arg_keys[1], (ROWS,), 0, CLASSES), jax.random.fold_in(arg_keys[1], 1), 0, CLASSES - 1).astype(jnp.int32),
        "leaf_ids": place_ends(jax.random.randint(arg_keys[2], (TREES, ROWS), 0, LEAVES), jax.random.fold_in(arg_keys[2], 1), 0, LEAVES - 1).astype(jnp.int32),
    }


step_size = 0.5
ridge_term = 1.0


def gradients(predict, labels):
    row_max = jnp.max(predict, axis=0, keepdims=True)
    exponent = jnp.exp(predict - row_max)
    probability = exponent / jnp.sum(exponent, axis=0, keepdims=True)
    classes = lax.broadcasted_iota(jnp.int32, predict.shape, 0)
    targets = (classes == labels[None, :]).astype(jnp.float32)
    gradient = (probability - targets).astype(jnp.bfloat16)
    hessian = (probability * (1.0 - probability)).astype(jnp.bfloat16)
    return gradient, hessian


def reference(predict, labels, leaf_ids):
    gradient, hessian = gradients(predict, labels)
    stacked = jnp.concatenate([gradient, hessian], axis=0).astype(jnp.float32).T

    def per_tree(tree_leaf):
        return jax.ops.segment_sum(stacked, tree_leaf, num_segments=LEAVES).T

    leaf_sums = lax.map(per_tree, leaf_ids)
    leaf_sums = jnp.transpose(leaf_sums, (1, 0, 2)).reshape(2 * CLASSES, TREES * LEAVES)
    leaf_values = -step_size * leaf_sums[:CLASSES] / (leaf_sums[CLASSES:] + ridge_term)
    value_rows = leaf_values.T
    offsets = (lax.broadcasted_iota(jnp.int32, (TREES, 1), 0) * LEAVES).astype(jnp.int32)
    flat_ids = (leaf_ids + offsets).astype(jnp.int32)

    def add_tree(running, tree_flat):
        return running + jnp.take(value_rows, tree_flat, axis=0), None

    update, unused = lax.scan(add_tree, jnp.zeros((ROWS, CLASSES), jnp.float32), flat_ids)
    return predict + update.T, leaf_values
```

```python
import functools
import jax, jax.numpy as jnp
from jax import lax
from jax.experimental import pallas as pl
from jax.experimental.pallas import tpu as pltpu
LEAVES=64
STEP=0.5
RIDGE=1.0
F32=jnp.float32; BF=jnp.bfloat16

def turned(b):
    return (b//4%4)*16+(b%4)*4+b//16

def softmax_piece(x, lab):
    m=jnp.max(x,axis=0,keepdims=True)
    e=jnp.exp(x-m)
    s=jnp.sum(e,axis=0,keepdims=True)
    p=e*(1.0/s)
    cls=lax.broadcasted_iota(jnp.int32,x.shape,0)
    g=jnp.where(cls==lab,p-1.0,p)
    h=p*(1.0-p)
    return g.astype(BF),h.astype(BF)

def one_hot(ids, iotas):
    f=ids.astype(F32)
    out=[]
    one=jnp.ones(iotas[0].shape,BF); zero=jnp.zeros(iotas[0].shape,BF)
    for t in range(f.shape[0]):
        r=jnp.broadcast_to(f[t:t+1,:],iotas[0].shape).astype(BF)
        for io in iotas:
            out.append(jnp.where(r==io,one,zero))
    return jnp.concatenate(out,axis=0)

def hist_kernel(UN, pred, lab, ids, out, xbuf, lbuf, ibuf, gh, acc, sems):
    classes,rows=pred.shape
    trees=ids.shape[0]
    NP=8; W=rows//NP
    cps=[pltpu.make_async_copy(pred.at[:,pl.ds(i*W,W)],xbuf.at[:,pl.ds(i*W,W)],sems.at[i]) for i in range(NP)]
    cl=pltpu.make_async_copy(lab,lbuf,sems.at[NP])
    ci=pltpu.make_async_copy(ids,ibuf,sems.at[NP+1])
    cl.start()
    for c in cps: c.start()
    ci.start()
    gh[...]=jnp.zeros_like(gh)
    cl.wait()
    for i in range(NP):
        cps[i].wait()
        @pl.loop(0,W,step=512)
        def _(o):
            sl=pl.ds(pl.multiple_of(i*W+o,512),512)
            g,h=softmax_piece(xbuf[:,sl],lbuf[:,sl])
            gh[0:classes,sl]=g
            gh[128:128+classes,sl]=h
    ci.wait()
    KT=256
    iotas=[(lax.broadcasted_iota(jnp.int32,(16,KT),0)+16*j).astype(F32).astype(BF) for j in range(4)]
    for c in range(trees//8):
        acc[...]=jnp.zeros_like(acc)
        @pl.loop(0,rows,step=KT*UN)
        def _(k):
            tot=None
            for u in range(UN):
                sl=pl.ds(pl.multiple_of(k+u*KT,KT),KT)
                oh=one_hot(ibuf[c*8:c*8+8,sl],iotas)
                d=lax.dot_general(oh,gh[:,sl],(((1,),(1,)),((),())),preferred_element_type=F32)
                tot=d if tot is None else tot+d
            acc[...]+=tot
        out[0,c*512:c*512+512,:]=acc[:,0:128]
        for b in range(64):
            to=c*512+turned(b)*8
            out[1,to:to+8,:]=acc[b*8:b*8+8,128:256]

def hist(pred,lab,ids,UN=8):
    classes,rows=pred.shape; trees=ids.shape[0]
    return pl.pallas_call(
        functools.partial(hist_kernel,UN),
        out_shape=jax.ShapeDtypeStruct((2,trees*LEAVES,128),F32),
        in_specs=[pl.BlockSpec(memory_space=pl.ANY)]*3,
        out_specs=pl.BlockSpec(memory_space=pltpu.VMEM),
        scratch_shapes=[pltpu.VMEM((classes,rows),F32),pltpu.VMEM((1,rows),jnp.int32),pltpu.VMEM((trees,rows),jnp.int32),
            pltpu.VMEM((256,rows),BF),pltpu.VMEM((512,256),F32),pltpu.SemaphoreType.DMA((10,))],
        compiler_params=pltpu.CompilerParams(vmem_limit_bytes=50<<20),
        name='hist',
    )(pred,lab,ids)

def apply_kernel(UN, v, pred, ids, out, own, vt, xbuf, ibuf, obuf, sems, osem):
    classes,rows=pred.shape
    trees=ids.shape[0]
    n=trees*LEAVES
    NP=8; W=rows//NP
    ci=pltpu.make_async_copy(ids,ibuf,sems.at[NP])
    ci.start()
    cps=[pltpu.make_async_copy(pred.at[:,pl.ds(i*W,W)],xbuf.at[:,pl.ds(i*W,W)],sems.at[i]) for i in range(NP)]
    for c in cps: c.start()
    for b in range(n//256):
        vt[:,b*256:b*256+256]=v[b*256:b*256+256,:].T[0:112,:].astype(BF)
    wide=own.shape[1]
    for b in range(wide//128):
        first=pl.multiple_of(lax.axis_index("leaf")*wide+b*128,128)
        own[:,b*128:b*128+128]=v[pl.ds(first,128),:].T[0:classes,:]
    ci.wait()
    KT=256
    iotas=[(lax.broadcasted_iota(jnp.int32,(16,KT),0)+16*j).astype(F32).astype(BF) for j in range(4)]
    outs=[]
    for i in range(NP):
        cps[i].wait()
        @pl.loop(0,W,step=KT)
        def _(o):
            sl=pl.ds(pl.multiple_of(i*W+o,KT),KT)
            tot=None
            for c in range(trees//8):
                oh=one_hot(ibuf[c*8:c*8+8,sl],iotas)
                d=jnp.dot(vt[:,c*512:c*512+512],oh,preferred_element_type=F32)
                tot=d if tot is None else tot+d
            obuf[:,sl]=xbuf[:,sl]+tot[0:classes]
        sl=pl.ds(i*W,W)
        oc=pltpu.make_async_copy(obuf.at[:,sl],out.at[:,sl],osem.at[i])
        oc.start(); outs.append(oc)
    for o in outs: o.wait()

def apply(v,pred,ids,UN=1):
    classes,rows=pred.shape; trees=ids.shape[0]
    return pl.pallas_call(
        functools.partial(apply_kernel,UN),
        out_shape=(jax.ShapeDtypeStruct(pred.shape,F32),jax.ShapeDtypeStruct((classes,trees*LEAVES//lax.axis_size("leaf")),F32)),
        in_specs=[pl.BlockSpec(memory_space=pltpu.VMEM)]+[pl.BlockSpec(memory_space=pl.ANY)]*2,
        out_specs=(pl.BlockSpec(memory_space=pl.ANY),pl.BlockSpec(memory_space=pltpu.VMEM)),
        scratch_shapes=[pltpu.VMEM((112,trees*LEAVES),BF),pltpu.VMEM((classes,rows),F32),pltpu.VMEM((trees,rows),jnp.int32),
            pltpu.VMEM((classes,rows),F32),pltpu.SemaphoreType.DMA((9,)),pltpu.SemaphoreType.DMA((8,))],
        compiler_params=pltpu.CompilerParams(vmem_limit_bytes=50<<20),
        name='apply',
    )(v,pred,ids)

from jax.sharding import Mesh
from jax.sharding import PartitionSpec as P

AXES = ("dp_0", "dp_1", "dp_2", "leaf")
ROWS_OF = (128, 32, 8)


def places():
    y, x, core, z = (lax.axis_index(name) for name in AXES)
    return x, y, z, core


def picks(axis):
    return (1 - axis) * (2 - axis) // 2, axis * (2 - axis), axis * (axis - 1) // 2


def along(axis, step):
    x, y, z, core = places()
    px, py, pz = picks(axis)
    q = px * x + py * y + pz * z
    move = (q + step) % 4 - q
    return (y + py * move, x + px * move, core, z + pz * move)


def spot(axis):
    x, y, z, core = places()
    px, py, pz = picks(axis)
    return px * x + py * y + pz * z


def greet():
    barrier = pltpu.get_barrier_semaphore()
    x, y, z, core = places()
    peers = [along(a, d) for a in range(3) for d in (1, 2, 3)] + [(y, x, 1 - core, z)]
    for peer in peers:
        pl.semaphore_signal(barrier, inc=1, device_id=peer, device_id_type=pl.DeviceIdType.MESH)
    pl.semaphore_wait(barrier, len(peers))


def stages(c, sums, held, bufs, send, recv):
    paired, part_a, got_a, part_b, got_b, part_c, got_c, both = bufs
    x, y, z, core = places()
    axes = [(2 * c + core + p) % 3 for p in range(3)]
    spots = [spot(a) for a in axes]
    base, values = c * 512, held.at[c]
    partner = (y, x, 1 - core, z)

    def copy(i, src, dst, peer):
        return pltpu.make_async_remote_copy(
            src_ref=src, dst_ref=dst, send_sem=send.at[c, i], recv_sem=recv.at[c, i],
            device_id=peer, device_id_type=pl.DeviceIdType.MESH)

    todo = []
    first = copy(0, sums.at[1 - core, pl.ds(base, 512)], paired.at[c], partner)
    todo.append([first])

    def halve(p, part, got):
        rows = ROWS_OF[p]
        out = []
        for d in (1, 2, 3):
            there = (spots[p] + d) % 4
            src = part.at[c, pl.ds(pl.multiple_of(there * rows, rows), rows)]
            out.append(copy(3 * p + d, src, got.at[c, d - 1], along(axes[p], d)))
        return out

    def mine(p, part, got):
        rows = ROWS_OF[p]
        held = part[c, pl.ds(pl.multiple_of(spots[p] * rows, rows), rows)]
        return (held + got[c, 0]) + (got[c, 1] + got[c, 2])

    a, b, e = halve(0, part_a, got_a), halve(1, part_b, got_b), halve(2, part_c, got_c)
    swap = [copy(10, both.at[c, core], both.at[c, core], partner)]
    at = [spots[0] * 128, spots[0] * 128 + spots[1] * 32]
    at.append(at[1] + spots[2] * 8)

    def spread(p):
        rows = ROWS_OF[p]
        where = values.at[pl.ds(pl.multiple_of(at[p], rows), rows)]
        return [copy(10 + 3 * (2 - p) + d, where, where, along(axes[p], d)) for d in (1, 2, 3)]

    def add_pair():
        part_a[c] = sums[core, base:base + 512] + paired[c]

    def add_a():
        part_b[c] = mine(0, part_a, got_a)

    def add_b():
        part_c[c] = mine(1, part_b, got_b)

    def add_c():
        both[c, core] = mine(2, part_c, got_c)

    def solve():
        held[c, pl.ds(pl.multiple_of(at[2], 8), 8)] = -STEP * both[c, 0] / (both[c, 1] + RIDGE)

    steps = [([first], add_pair), (a, add_a), (b, add_b), (e, add_c), (swap, solve),
             (spread(2), None), (spread(1), None), (spread(0), None)]
    return steps


def sum_kernel(sums, values, *scratch):
    held, bufs, send, recv = scratch[0], scratch[1:-2], scratch[-2], scratch[-1]
    greet()
    chunks = [stages(c, sums, held, bufs, send, recv) for c in range(4)]
    for s in range(len(chunks[0])):
        for steps in chunks:
            for copy in steps[s][0]:
                copy.start()
        for steps in chunks:
            for copy in steps[s][0]:
                copy.wait_recv()
            if steps[s][1] is not None:
                steps[s][1]()
    core = lax.axis_index(AXES[2])
    for c in range(4):
        for b in range(64):
            place = pl.multiple_of((b + core * (turned(b) - b)) * 8, 8)
            values[c * 512 + b * 8:c * 512 + b * 8 + 8] = held[c, pl.ds(place, 8)]
    for steps in chunks:
        for copies, _ in steps:
            for copy in copies:
                copy.wait_send()


def total(sums):
    n = sums.shape[1]
    k = n // 512
    return pl.pallas_call(
        sum_kernel,
        out_shape=jax.ShapeDtypeStruct((n, 128), F32),
        in_specs=[pl.BlockSpec(memory_space=pltpu.VMEM)],
        out_specs=pl.BlockSpec(memory_space=pltpu.VMEM),
        scratch_shapes=[
            pltpu.VMEM((k, 512, 128), F32), pltpu.VMEM((k, 512, 128), F32), pltpu.VMEM((k, 512, 128), F32), pltpu.VMEM((k, 3, 128, 128), F32),
            pltpu.VMEM((k, 128, 128), F32), pltpu.VMEM((k, 3, 32, 128), F32),
            pltpu.VMEM((k, 32, 128), F32), pltpu.VMEM((k, 3, 8, 128), F32), pltpu.VMEM((k, 2, 8, 128), F32),
            pltpu.SemaphoreType.DMA((k, 20)), pltpu.SemaphoreType.DMA((k, 20)),
        ],
        compiler_params=pltpu.CompilerParams(collective_id=0, has_side_effects=True, vmem_limit_bytes=24 << 20),
        name='total',
    )(sums)


def shards(predict, labels, leaf_ids):
    sums = hist(predict, labels[None, :], leaf_ids)
    values = total(sums)
    return apply(values, predict, leaf_ids)


def solution(mesh):
    finer = Mesh(mesh.devices.reshape(4, 4, 2, mesh.shape["leaf"]), AXES)
    in_specs = (P(None, AXES), P(AXES), P(None, AXES))
    out_specs = (P(None, AXES), P(None, "leaf"))
    return jax.shard_map(shards, mesh=finer, in_specs=in_specs, out_specs=out_specs, check_vma=False)
```

```python
import jax
import jax.numpy as jnp
from jax import lax
from jax.experimental import pallas as pl
from jax.experimental.pallas import tpu as pltpu
from jax.sharding import Mesh
from jax.sharding import PartitionSpec as P

F32, BF16 = jnp.float32, jnp.bfloat16
LEAVES = 64
AXES = ("dp_0", "dp_1", "dp_2", "leaf")
TREES_AT_ONCE = 8
WIDE = TREES_AT_ONCE * LEAVES
LANES = 128
ROWS_OF = (128, 32, 8)
COPIES = 23
TILE = 256
PIECES = 8

step_size = 0.5
ridge_term = 1.0


def turned(block):
    return (block // 4 % 4) * 16 + (block % 4) * 4 + block // 16


def places():
    y, x, core, z = (lax.axis_index(name) for name in AXES)
    return x, y, z, core


def picks(axis):
    return (1 - axis) * (2 - axis) // 2, axis * (2 - axis), axis * (axis - 1) // 2


def spot(axis):
    x, y, z, _ = places()
    px, py, pz = picks(axis)
    return px * x + py * y + pz * z


def along(axis, step, core):
    x, y, z, _ = places()
    px, py, pz = picks(axis)
    q = spot(axis)
    move = (q + step) % 4 - q
    return (y + py * move, x + px * move, core, z + pz * move)


def partner():
    x, y, z, core = places()
    return (y, x, 1 - core, z)


def greeted():
    core = lax.axis_index(AXES[2])
    return [along(a, d, k) for a in range(3) for d in (1, 2, 3) for k in (core, 1 - core)] + [partner()]


def greet():
    barrier = pltpu.get_barrier_semaphore()
    for peer in greeted():
        pl.semaphore_signal(barrier, inc=1, device_id=peer, device_id_type=pl.DeviceIdType.MESH)


def wait_for_all():
    pl.semaphore_wait(pltpu.get_barrier_semaphore(), len(greeted()))


class Exchange:
    def __init__(self, c, sums, held, bufs, send, recv):
        paired, part_a, got_a, part_b, got_b, part_c, last = bufs
        core = lax.axis_index(AXES[2])
        axes = [(2 * c + core + p) % 3 for p in range(3)]
        spots = [spot(a) for a in axes]
        base, values = c * WIDE, held.at[c]

        def copy(i, src, dst, peer):
            return pltpu.make_async_remote_copy(
                src_ref=src,
                dst_ref=dst,
                send_sem=send.at[c, i],
                recv_sem=recv.at[c, i],
                device_id=peer,
                device_id_type=pl.DeviceIdType.MESH,
            )

        def block(p, step):
            there = (spots[p] + step) % 4
            return pl.ds(pl.multiple_of(there * ROWS_OF[p], ROWS_OF[p]), ROWS_OF[p])

        def halve(p, part, got):
            return [
                copy(3 * p + d, part.at[c, block(p, d)], got.at[c, d - 1], along(axes[p], d, core))
                for d in (1, 2, 3)
            ]

        def mine(p, part, got):
            return (part[c, block(p, 0)] + got[c, 0]) + (got[c, 1] + got[c, 2])

        at = [spots[0] * 128, spots[0] * 128 + spots[1] * 32]
        at.append(at[1] + spots[2] * 8)

        def spread(p):
            where = values.at[pl.ds(pl.multiple_of(at[p], ROWS_OF[p]), ROWS_OF[p])]
            return [copy(14 + 3 * (2 - p) + d - 1, where, where, along(axes[p], d, core)) for d in (1, 2, 3)]

        finals = [copy(7, part_c.at[c, block(2, 0)], last.at[c, core, 0], partner())]
        for d in (1, 2, 3):
            src, dst = part_c.at[c, block(2, d)], last.at[c, core, d]
            finals.append(copy(7 + d, src, dst, along(axes[2], d, core)))
            finals.append(copy(10 + d, src, dst, along(axes[2], d, 1 - core)))

        def add_pair():
            part_a[c] = sums[core, base : base + WIDE] + paired[c]

        def add_a():
            part_b[c] = mine(0, part_a, got_a)

        def add_b():
            part_c[c] = mine(1, part_b, got_b)
            last[c, core, 0] = part_c[c, block(2, 0)]

        def solve():
            grad, hess = (
                (last[c, k, 0] + last[c, k, 1]) + (last[c, k, 2] + last[c, k, 3]) for k in (0, 1)
            )
            held[c, pl.ds(pl.multiple_of(at[2], 8), 8)] = -step_size * grad / (hess + ridge_term)

        first = copy(0, sums.at[1 - core, pl.ds(base, WIDE)], paired.at[c], partner())
        self.steps = [
            ([first], add_pair),
            (halve(0, part_a, got_a), add_a),
            (halve(1, part_b, got_b), add_b),
            (finals, solve),
            (spread(2), None),
            (spread(1), None),
            (spread(0), None),
        ]
        self.now = 0

    @property
    def done(self):
        return self.now == len(self.steps)

    def start(self):
        for copy in self.steps[self.now][0]:
            copy.start()

    def advance(self):
        copies, then = self.steps[self.now]
        for copy in copies:
            copy.wait_recv()
        if then is not None:
            then()
        self.now += 1
        if not self.done:
            self.start()

    def settle(self):
        for copies, _ in self.steps:
            for copy in copies:
                copy.wait_send()


def gradients(predict, labels):
    exponent = jnp.exp(predict - jnp.max(predict, axis=0, keepdims=True))
    probability = exponent * (1.0 / jnp.sum(exponent, axis=0, keepdims=True))
    classes = lax.broadcasted_iota(jnp.int32, predict.shape, 0)
    gradient = jnp.where(classes == labels, probability - 1.0, probability)
    return gradient.astype(BF16), (probability * (1.0 - probability)).astype(BF16)


def leaf_slots(width):
    return [(lax.broadcasted_iota(jnp.int32, (16, width), 0) + 16 * j).astype(F32).astype(BF16) for j in range(4)]


def one_hot(ids, slots):
    shape = slots[0].shape
    one, zero = jnp.ones(shape, BF16), jnp.zeros(shape, BF16)
    ids = ids.astype(F32)
    rows = []
    for t in range(ids.shape[0]):
        held = jnp.broadcast_to(ids[t : t + 1], shape).astype(BF16)
        rows += [jnp.where(held == slot, one, zero) for slot in slots]
    return jnp.concatenate(rows, axis=0)


def chunk_sums(c, ids, stacked, acc, sums, unroll=8):
    rows = ids.shape[1]
    slots = leaf_slots(TILE)
    acc[...] = jnp.zeros_like(acc)

    @pl.loop(0, rows, step=TILE * unroll)
    def _(first):
        total = None
        for u in range(unroll):
            cols = pl.ds(pl.multiple_of(first + u * TILE, TILE), TILE)
            matches = one_hot(ids[c * TREES_AT_ONCE : (c + 1) * TREES_AT_ONCE, cols], slots)
            part = lax.dot_general(
                matches, stacked[:, cols], (((1,), (1,)), ((), ())), preferred_element_type=F32
            )
            total = part if total is None else total + part
        acc[...] += total

    base = c * WIDE
    sums[0, base : base + WIDE] = acc[:, :LANES]
    for b in range(64):
        to = base + turned(b) * 8
        sums[1, to : to + 8] = acc[b * 8 : b * 8 + 8, LANES:]


def in_order(c, held, values):
    core = lax.axis_index(AXES[2])
    for b in range(64):
        place = pl.multiple_of((b + core * (turned(b) - b)) * 8, 8)
        values[c * WIDE + b * 8 : c * WIDE + b * 8 + 8] = held[c, pl.ds(place, 8)]


def class_major(values, first, table):
    for b in range(WIDE // LANES):
        block = values[first + b * LANES : first + (b + 1) * LANES]
        table[:, b * LANES : (b + 1) * LANES] = block.T[: table.shape[0]].astype(BF16)


def grow_kernel(predict, labels, ids, carried, values, *scratch):
    lbuf, ibuf, stacked, acc, table, sums, held = scratch[:7]
    bufs, send, recv, sems = scratch[7:-3], *scratch[-3:]
    classes, rows = predict.shape
    width = rows // PIECES
    greet()
    reads = []
    for i in range(PIECES):
        cols = pl.ds(i * width, width)
        reads.append(pltpu.make_async_copy(predict.at[:, cols], carried.at[:, cols], sems.at[i]))
    labels_read = pltpu.make_async_copy(labels, lbuf, sems.at[PIECES])
    ids_read = pltpu.make_async_copy(ids, ibuf, sems.at[PIECES + 1])
    labels_read.start()
    for read in reads:
        read.start()
    ids_read.start()
    for k in (0, 1):
        stacked[k * LANES + 96 : (k + 1) * LANES] = jnp.zeros((LANES - 96, rows), BF16)
    labels_read.wait()
    for i in range(PIECES):
        reads[i].wait()

        @pl.loop(0, width, step=512)
        def _(first):
            cols = pl.ds(pl.multiple_of(i * width + first, 512), 512)
            gradient, hessian = gradients(carried[:, cols], lbuf[:, cols])
            stacked[:classes, cols] = gradient
            stacked[LANES : LANES + classes, cols] = hessian

    ids_read.wait()
    chunks = [Exchange(c, sums, held, bufs, send, recv) for c in range(ids.shape[0] // TREES_AT_ONCE)]

    def apply(c):
        in_order(c, held, values)
        class_major(values, c * WIDE, table)
        slots = leaf_slots(TILE)

        @pl.loop(0, rows, step=2 * TILE)
        def _(first):
            for u in range(2):
                cols = pl.ds(pl.multiple_of(first + u * TILE, TILE), TILE)
                matches = one_hot(ibuf[c * TREES_AT_ONCE : (c + 1) * TREES_AT_ONCE, cols], slots)
                update = jnp.dot(table[...], matches, preferred_element_type=F32)
                carried[:, cols] += update[:classes]

    newest = len(chunks) - 1
    for c in range(len(chunks)):
        chunk_sums(c, ibuf, stacked, acc, sums)
        if c == 0:
            wait_for_all()
        chunks[c].start()
        for older in reversed(range(c)):
            if c < newest or older == newest - 1:
                chunks[older].advance()
    applied = 0
    while not chunks[newest].done:
        chunks[newest].advance()
        for older in reversed(range(newest)):
            if not chunks[older].done:
                chunks[older].advance()
        if applied < newest and chunks[applied].done:
            apply(applied)
            applied += 1
    while applied < newest:
        apply(applied)
        applied += 1
    in_order(newest, held, values)
    for chunk in chunks:
        chunk.settle()


def grow(predict, labels, ids):
    classes, rows = predict.shape
    leaves = ids.shape[0] * LEAVES
    k = leaves // WIDE
    pinned = [pltpu.with_memory_space_constraint(a, pltpu.HBM) for a in (predict, labels, ids)]
    return pl.pallas_call(
        grow_kernel,
        out_shape=(jax.ShapeDtypeStruct(predict.shape, F32), jax.ShapeDtypeStruct((leaves, LANES), F32)),
        in_specs=[pl.BlockSpec(memory_space=pltpu.HBM)] * 3,
        out_specs=(pl.BlockSpec(memory_space=pltpu.VMEM), pl.BlockSpec(memory_space=pltpu.VMEM)),
        scratch_shapes=[
            pltpu.VMEM((1, rows), jnp.int32),
            pltpu.VMEM(ids.shape, jnp.int32),
            pltpu.VMEM((2 * LANES, rows), BF16),
            pltpu.VMEM((WIDE, 2 * LANES), F32),
            pltpu.VMEM((112, WIDE), BF16),
            pltpu.VMEM((2, leaves, LANES), F32),
            pltpu.VMEM((k, WIDE, LANES), F32),
            pltpu.VMEM((k, WIDE, LANES), F32),
            pltpu.VMEM((k, WIDE, LANES), F32),
            pltpu.VMEM((k, 3, 128, LANES), F32),
            pltpu.VMEM((k, 128, LANES), F32),
            pltpu.VMEM((k, 3, 32, LANES), F32),
            pltpu.VMEM((k, 32, LANES), F32),
            pltpu.VMEM((k, 2, 4, 8, LANES), F32),
            pltpu.SemaphoreType.DMA((k, COPIES)),
            pltpu.SemaphoreType.DMA((k, COPIES)),
            pltpu.SemaphoreType.DMA((PIECES + 2,)),
        ],
        compiler_params=pltpu.CompilerParams(
            collective_id=0, has_side_effects=True, vmem_limit_bytes=40 << 20
        ),
        name="grow",
    )(*pinned)


def finish_kernel(values, carried, ids, out, own, table, ibuf, obuf, sems, ids_sem):
    classes, rows = carried.shape
    width = rows // PIECES
    first_id = ids.shape[0] - TREES_AT_ONCE
    ids_read = pltpu.make_async_copy(ids.at[pl.ds(first_id, TREES_AT_ONCE)], ibuf, ids_sem)
    ids_read.start()
    class_major(values, values.shape[0] - WIDE, table)
    ids_read.wait()
    slots = leaf_slots(TILE)
    writes = []
    for i in range(PIECES):

        @pl.loop(0, width, step=2 * TILE)
        def _(first):
            for u in range(2):
                cols = pl.ds(pl.multiple_of(i * width + first + u * TILE, TILE), TILE)
                matches = one_hot(ibuf[:, cols], slots)
                update = jnp.dot(table[...], matches, preferred_element_type=F32)
                obuf[:, cols] = carried[:, cols] + update[:classes]

        cols = pl.ds(i * width, width)
        writes.append(pltpu.make_async_copy(obuf.at[:, cols], out.at[:, cols], sems.at[i]))
        writes[-1].start()
    own_width = own.shape[1]
    for b in range(own_width // LANES):
        first = pl.multiple_of(lax.axis_index("leaf") * own_width + b * LANES, LANES)
        own[:, b * LANES : (b + 1) * LANES] = values[pl.ds(first, LANES)].T[:classes]
    for write in writes:
        write.wait()


def finish(values, carried, ids):
    classes, rows = carried.shape
    own_width = values.shape[0] // lax.axis_size("leaf")
    return pl.pallas_call(
        finish_kernel,
        out_shape=(
            jax.ShapeDtypeStruct(carried.shape, F32),
            jax.ShapeDtypeStruct((classes, own_width), F32),
        ),
        in_specs=[
            pl.BlockSpec(memory_space=pltpu.VMEM),
            pl.BlockSpec(memory_space=pltpu.VMEM),
            pl.BlockSpec(memory_space=pl.ANY),
        ],
        out_specs=(pl.BlockSpec(memory_space=pl.ANY), pl.BlockSpec(memory_space=pltpu.VMEM)),
        scratch_shapes=[
            pltpu.VMEM((112, WIDE), BF16),
            pltpu.VMEM((TREES_AT_ONCE, rows), jnp.int32),
            pltpu.VMEM((classes, rows), F32),
            pltpu.SemaphoreType.DMA((PIECES,)),
            pltpu.SemaphoreType.DMA,
        ],
        compiler_params=pltpu.CompilerParams(vmem_limit_bytes=24 << 20),
        name="finish",
    )(values, carried, ids)


def shards(predict, labels, leaf_ids):
    carried, values = grow(predict, labels[None, :], leaf_ids)
    return finish(values, carried, leaf_ids)


def solution(mesh):
    finer = Mesh(mesh.devices.reshape(4, 4, 2, mesh.shape["leaf"]), AXES)
    in_specs = (P(None, AXES), P(AXES), P(None, AXES))
    out_specs = (P(None, AXES), P(None, "leaf"))
    return jax.shard_map(shards, mesh=finer, in_specs=in_specs, out_specs=out_specs, check_vma=False)
```

```python
import jax
import jax.numpy as jnp
from jax import lax
from jax.experimental import pallas as pl
from jax.experimental.pallas import tpu as pltpu
from jax.sharding import Mesh
from jax.sharding import PartitionSpec as P

F32, BF16 = jnp.float32, jnp.bfloat16
LEAVES = 64
AXES = ("dp_0", "dp_1", "dp_2", "leaf")
TREES_AT_ONCE = 8
WIDE = TREES_AT_ONCE * LEAVES
LANES = 128
ROWS_OF = (128, 32, 8)
COPIES = 23
TILE = 256
PIECES = 8
APPLY = 16
WRITES = 4

step_size = 0.5
ridge_term = 1.0


def turned(block):
    return (block // 4 % 4) * 16 + (block % 4) * 4 + block // 16


def places():
    y, x, core, z = (lax.axis_index(name) for name in AXES)
    return x, y, z, core


def picks(axis):
    return (1 - axis) * (2 - axis) // 2, axis * (2 - axis), axis * (axis - 1) // 2


def spot(axis):
    x, y, z, _ = places()
    px, py, pz = picks(axis)
    return px * x + py * y + pz * z


def along(axis, step, core):
    x, y, z, _ = places()
    px, py, pz = picks(axis)
    q = spot(axis)
    move = (q + step) % 4 - q
    return (y + py * move, x + px * move, core, z + pz * move)


def partner():
    x, y, z, core = places()
    return (y, x, 1 - core, z)


def greeted():
    core = lax.axis_index(AXES[2])
    return [along(a, d, k) for a in range(3) for d in (1, 2, 3) for k in (core, 1 - core)] + [partner()]


def greet():
    barrier = pltpu.get_barrier_semaphore()
    for peer in greeted():
        pl.semaphore_signal(barrier, inc=1, device_id=peer, device_id_type=pl.DeviceIdType.MESH)


def wait_for_all():
    pl.semaphore_wait(pltpu.get_barrier_semaphore(), len(greeted()))


class Exchange:
    def __init__(self, c, sums, held, bufs, send, recv):
        paired, part_a, got_a, part_b, got_b, part_c, last = bufs
        core = lax.axis_index(AXES[2])
        axes = [(2 * c + core + p) % 3 for p in range(3)]
        spots = [spot(a) for a in axes]
        base, values = c * WIDE, held.at[c]

        def copy(i, src, dst, peer):
            return pltpu.make_async_remote_copy(
                src_ref=src,
                dst_ref=dst,
                send_sem=send.at[c, i],
                recv_sem=recv.at[c, i],
                device_id=peer,
                device_id_type=pl.DeviceIdType.MESH,
            )

        def block(p, step):
            there = (spots[p] + step) % 4
            return pl.ds(pl.multiple_of(there * ROWS_OF[p], ROWS_OF[p]), ROWS_OF[p])

        def halve(p, part, got):
            return [
                copy(3 * p + d, part.at[c, block(p, d)], got.at[c, d - 1], along(axes[p], d, core))
                for d in (1, 2, 3)
            ]

        def mine(p, part, got):
            return (part[c, block(p, 0)] + got[c, 0]) + (got[c, 1] + got[c, 2])

        at = [spots[0] * 128, spots[0] * 128 + spots[1] * 32]
        at.append(at[1] + spots[2] * 8)

        def spread(p):
            where = values.at[pl.ds(pl.multiple_of(at[p], ROWS_OF[p]), ROWS_OF[p])]
            return [copy(14 + 3 * (2 - p) + d - 1, where, where, along(axes[p], d, core)) for d in (1, 2, 3)]

        finals = [copy(7, part_c.at[c, block(2, 0)], last.at[c, core, 0], partner())]
        for d in (1, 2, 3):
            src, dst = part_c.at[c, block(2, d)], last.at[c, core, d]
            finals.append(copy(7 + d, src, dst, along(axes[2], d, core)))
            finals.append(copy(10 + d, src, dst, along(axes[2], d, 1 - core)))

        def add_pair():
            part_a[c] = sums[core, base : base + WIDE] + paired[c]

        def add_a():
            part_b[c] = mine(0, part_a, got_a)

        def add_b():
            part_c[c] = mine(1, part_b, got_b)
            last[c, core, 0] = part_c[c, block(2, 0)]

        def solve():
            grad, hess = (
                (last[c, k, 0] + last[c, k, 1]) + (last[c, k, 2] + last[c, k, 3]) for k in (0, 1)
            )
            held[c, pl.ds(pl.multiple_of(at[2], 8), 8)] = -step_size * grad / (hess + ridge_term)

        first = copy(0, sums.at[1 - core, pl.ds(base, WIDE)], paired.at[c], partner())
        self.steps = [
            ([first], add_pair),
            (halve(0, part_a, got_a), add_a),
            (halve(1, part_b, got_b), add_b),
            (finals, solve),
            (spread(2), None),
            (spread(1), None),
            (spread(0), None),
        ]
        self.now = 0

    @property
    def done(self):
        return self.now == len(self.steps)

    def start(self):
        for copy in self.steps[self.now][0]:
            copy.start()

    def advance(self):
        copies, then = self.steps[self.now]
        for copy in copies:
            copy.wait_recv()
        if then is not None:
            then()
        self.now += 1
        if not self.done:
            self.start()

    def settle(self):
        for copies, _ in self.steps:
            for copy in copies:
                copy.wait_send()


def gradients(predict, labels):
    exponent = jnp.exp(predict - jnp.max(predict, axis=0, keepdims=True))
    probability = exponent * (1.0 / jnp.sum(exponent, axis=0, keepdims=True))
    classes = lax.broadcasted_iota(jnp.int32, predict.shape, 0)
    gradient = jnp.where(classes == labels, probability - 1.0, probability)
    return gradient.astype(BF16), (probability * (1.0 - probability)).astype(BF16)


def leaf_slots(width):
    return [(lax.broadcasted_iota(jnp.int32, (16, width), 0) + 16 * j).astype(F32).astype(BF16) for j in range(4)]


def one_hot(ids, slots):
    shape = slots[0].shape
    one, zero = jnp.ones(shape, BF16), jnp.zeros(shape, BF16)
    ids = ids.astype(F32)
    rows = []
    for t in range(ids.shape[0]):
        held = jnp.broadcast_to(ids[t : t + 1], shape).astype(BF16)
        rows += [jnp.where(held == slot, one, zero) for slot in slots]
    return jnp.concatenate(rows, axis=0)


def chunk_sums(c, half, ids, stacked, acc, sums, unroll=8):
    rows = ids.shape[1] // 2
    slots = leaf_slots(TILE)
    if half == 0:
        acc[...] = jnp.zeros_like(acc)

    @pl.loop(half * rows, (half + 1) * rows, step=TILE * unroll)
    def _(first):
        total = None
        for u in range(unroll):
            cols = pl.ds(pl.multiple_of(first + u * TILE, TILE), TILE)
            matches = one_hot(ids[c * TREES_AT_ONCE : (c + 1) * TREES_AT_ONCE, cols], slots)
            part = lax.dot_general(
                matches, stacked[:, cols], (((1,), (1,)), ((), ())), preferred_element_type=F32
            )
            total = part if total is None else total + part
        acc[...] += total

    if half == 1:
        base = c * WIDE
        sums[0, base : base + WIDE] = acc[:, :LANES]
        for b in range(64):
            to = base + turned(b) * 8
            sums[1, to : to + 8] = acc[b * 8 : b * 8 + 8, LANES:]


def in_order(c, held, values):
    core = lax.axis_index(AXES[2])
    for b in range(64):
        place = pl.multiple_of((b + core * (turned(b) - b)) * 8, 8)
        values[c * WIDE + b * 8 : c * WIDE + b * 8 + 8] = held[c, pl.ds(place, 8)]


def class_major(values, first, table):
    for b in range(WIDE // LANES):
        block = values[first + b * LANES : first + (b + 1) * LANES]
        table[:, b * LANES : (b + 1) * LANES] = block.T[: table.shape[0]].astype(BF16)


def grow_kernel(predict, labels, ids, carried, values, *scratch):
    lbuf, ibuf, stacked, acc, table, sums, held = scratch[:7]
    bufs, send, recv, sems = scratch[7:-3], *scratch[-3:]
    classes, rows = predict.shape
    width = rows // PIECES
    greet()
    reads = []
    for i in range(PIECES):
        cols = pl.ds(i * width, width)
        reads.append(pltpu.make_async_copy(predict.at[:, cols], carried.at[:, cols], sems.at[i]))
    labels_read = pltpu.make_async_copy(labels, lbuf, sems.at[PIECES])
    ids_read = pltpu.make_async_copy(ids, ibuf, sems.at[PIECES + 1])
    labels_read.start()
    for read in reads:
        read.start()
    ids_read.start()
    for k in (0, 1):
        stacked[k * LANES + 96 : (k + 1) * LANES] = jnp.zeros((LANES - 96, rows), BF16)
    labels_read.wait()
    for i in range(PIECES):
        reads[i].wait()

        @pl.loop(0, width, step=512)
        def _(first):
            cols = pl.ds(pl.multiple_of(i * width + first, 512), 512)
            gradient, hessian = gradients(carried[:, cols], lbuf[:, cols])
            stacked[:classes, cols] = gradient
            stacked[LANES : LANES + classes, cols] = hessian

    ids_read.wait()
    chunks = [Exchange(c, sums, held, bufs, send, recv) for c in range(ids.shape[0] // TREES_AT_ONCE)]

    def apply(c):
        in_order(c, held, values)
        class_major(values, c * WIDE, table)
        slots = leaf_slots(TILE)

        @pl.loop(0, rows, step=APPLY * TILE)
        def _(first):
            for u in range(APPLY):
                cols = pl.ds(pl.multiple_of(first + u * TILE, TILE), TILE)
                matches = one_hot(ibuf[c * TREES_AT_ONCE : (c + 1) * TREES_AT_ONCE, cols], slots)
                update = jnp.dot(table[...], matches, preferred_element_type=F32)
                carried[:, cols] += update[:classes]

    newest = len(chunks) - 1
    for c in range(newest + 1):
        chunk_sums(c, 0, ibuf, stacked, acc, sums)
        if c >= 1:
            chunks[c - 1].advance()
        chunk_sums(c, 1, ibuf, stacked, acc, sums)
        if c == 0:
            wait_for_all()
        if c >= 2:
            chunks[c - 2].advance()
        chunks[c].start()
    while not chunks[newest].done:
        for c in (newest, 0, *range(newest - 1, 0, -1)):
            if not chunks[c].done:
                chunks[c].advance()
                if chunks[c].done and c < newest:
                    apply(c)
    in_order(newest, held, values)
    for chunk in chunks:
        chunk.settle()


def grow(predict, labels, ids):
    classes, rows = predict.shape
    leaves = ids.shape[0] * LEAVES
    k = leaves // WIDE
    pinned = [pltpu.with_memory_space_constraint(a, pltpu.HBM) for a in (predict, labels, ids)]
    return pl.pallas_call(
        grow_kernel,
        out_shape=(jax.ShapeDtypeStruct(predict.shape, F32), jax.ShapeDtypeStruct((leaves, LANES), F32)),
        in_specs=[pl.BlockSpec(memory_space=pltpu.HBM)] * 3,
        out_specs=(pl.BlockSpec(memory_space=pltpu.VMEM), pl.BlockSpec(memory_space=pltpu.VMEM)),
        scratch_shapes=[
            pltpu.VMEM((1, rows), jnp.int32),
            pltpu.VMEM(ids.shape, jnp.int32),
            pltpu.VMEM((2 * LANES, rows), BF16),
            pltpu.VMEM((WIDE, 2 * LANES), F32),
            pltpu.VMEM((112, WIDE), BF16),
            pltpu.VMEM((2, leaves, LANES), F32),
            pltpu.VMEM((k, WIDE, LANES), F32),
            pltpu.VMEM((k, WIDE, LANES), F32),
            pltpu.VMEM((k, WIDE, LANES), F32),
            pltpu.VMEM((k, 3, 128, LANES), F32),
            pltpu.VMEM((k, 128, LANES), F32),
            pltpu.VMEM((k, 3, 32, LANES), F32),
            pltpu.VMEM((k, 32, LANES), F32),
            pltpu.VMEM((k, 2, 4, 8, LANES), F32),
            pltpu.SemaphoreType.DMA((k, COPIES)),
            pltpu.SemaphoreType.DMA((k, COPIES)),
            pltpu.SemaphoreType.DMA((PIECES + 2,)),
        ],
        compiler_params=pltpu.CompilerParams(
            collective_id=0, has_side_effects=True, vmem_limit_bytes=40 << 20
        ),
        name="grow",
    )(*pinned)


def finish_kernel(values, carried, ids, out, own, table, ibuf, obuf, sems, ids_sem):
    classes, rows = carried.shape
    width = rows // WRITES
    first_id = ids.shape[0] - TREES_AT_ONCE
    ids_read = pltpu.make_async_copy(ids.at[pl.ds(first_id, TREES_AT_ONCE)], ibuf, ids_sem)
    ids_read.start()
    class_major(values, values.shape[0] - WIDE, table)
    ids_read.wait()
    slots = leaf_slots(TILE)
    writes = []
    for i in range(WRITES):
        for u in range(width // TILE):
            cols = pl.ds(i * width + u * TILE, TILE)
            update = jnp.dot(table[...], one_hot(ibuf[:, cols], slots), preferred_element_type=F32)
            obuf[:, cols] = carried[:, cols] + update[:classes]
        cols = pl.ds(i * width, width)
        writes.append(pltpu.make_async_copy(obuf.at[:, cols], out.at[:, cols], sems.at[i]))
        writes[-1].start()
    own_width = own.shape[1]
    for b in range(own_width // LANES):
        first = pl.multiple_of(lax.axis_index("leaf") * own_width + b * LANES, LANES)
        own[:, b * LANES : (b + 1) * LANES] = values[pl.ds(first, LANES)].T[:classes]
    for write in writes:
        write.wait()


def finish(values, carried, ids):
    classes, rows = carried.shape
    own_width = values.shape[0] // lax.axis_size("leaf")
    return pl.pallas_call(
        finish_kernel,
        out_shape=(
            jax.ShapeDtypeStruct(carried.shape, F32),
            jax.ShapeDtypeStruct((classes, own_width), F32),
        ),
        in_specs=[
            pl.BlockSpec(memory_space=pltpu.VMEM),
            pl.BlockSpec(memory_space=pltpu.VMEM),
            pl.BlockSpec(memory_space=pl.ANY),
        ],
        out_specs=(pl.BlockSpec(memory_space=pl.ANY), pl.BlockSpec(memory_space=pltpu.VMEM)),
        scratch_shapes=[
            pltpu.VMEM((112, WIDE), BF16),
            pltpu.VMEM((TREES_AT_ONCE, rows), jnp.int32),
            pltpu.VMEM((classes, rows), F32),
            pltpu.SemaphoreType.DMA((WRITES,)),
            pltpu.SemaphoreType.DMA,
        ],
        compiler_params=pltpu.CompilerParams(vmem_limit_bytes=24 << 20),
        name="finish",
    )(values, carried, ids)


def shards(predict, labels, leaf_ids):
    carried, values = grow(predict, labels[None, :], leaf_ids)
    return finish(values, carried, leaf_ids)


def solution(mesh):
    finer = Mesh(mesh.devices.reshape(4, 4, 2, mesh.shape["leaf"]), AXES)
    in_specs = (P(None, AXES), P(AXES), P(None, AXES))
    out_specs = (P(None, AXES), P(None, "leaf"))
    return jax.shard_map(shards, mesh=finer, in_specs=in_specs, out_specs=out_specs, check_vma=False)
```

```python
import jax
import jax.numpy as jnp
from jax import lax
from jax.experimental import pallas as pl
from jax.experimental.pallas import tpu as pltpu
from jax.sharding import Mesh
from jax.sharding import PartitionSpec as P

F32, BF16 = jnp.float32, jnp.bfloat16
LEAVES = 64
AXES = ("dp_0", "dp_1", "dp_2", "leaf")
TREES_AT_ONCE = 8
WIDE = TREES_AT_ONCE * LEAVES
LANES = 128
CHUNKS = (8, 8, 8, 8)
COPIES = 24
TILE = 256
PIECES = 8
APPLY = 16
WRITES = 4
UNROLL = 16
HALF_US, APPLY_US, EARLY_US = 1.15, 1.9, 0.3

step_size = 0.5
ridge_term = 1.0


def turned(block):
    return (block // 4 % 4) * 16 + (block % 4) * 4 + block // 16


def places():
    y, x, core, z = (lax.axis_index(name) for name in AXES)
    return x, y, z, core


def picks(axis):
    return (1 - axis) * (2 - axis) // 2, axis * (2 - axis), axis * (axis - 1) // 2


def spot(axis):
    x, y, z, _ = places()
    px, py, pz = picks(axis)
    return px * x + py * y + pz * z


def along(axis, step, core):
    x, y, z, _ = places()
    px, py, pz = picks(axis)
    q = spot(axis)
    move = (q + step) % 4 - q
    return (y + py * move, x + px * move, core, z + pz * move)


def partner():
    x, y, z, core = places()
    return (y, x, 1 - core, z)


def greeted():
    core = lax.axis_index(AXES[2])
    return [along(a, d, k) for a in range(3) for d in (1, 2, 3) for k in (core, 1 - core)] + [partner()]


def greet():
    barrier = pltpu.get_barrier_semaphore()
    for peer in greeted():
        pl.semaphore_signal(barrier, inc=1, device_id=peer, device_id_type=pl.DeviceIdType.MESH)


def wait_for_all():
    pl.semaphore_wait(pltpu.get_barrier_semaphore(), len(greeted()))


class Exchange:
    def __init__(self, c, trees, base, sums, held, bufs, send, recv):
        paired, part_a, got_a, part_b, got_b, part_c, last = bufs
        core = lax.axis_index(AXES[2])
        axes = [(c + core + p) % 3 for p in range(3)]
        spots = [spot(a) for a in axes]
        size = trees * LEAVES
        rows_of = [size // 4, size // 16, size // 64]
        whole = pl.ds(base, size)
        starts = [base, base // 4, base // 16, base // 64]

        def copy(i, src, dst, peer, lands=None):
            return pltpu.make_async_remote_copy(
                src_ref=src,
                dst_ref=dst,
                send_sem=send.at[c, i],
                recv_sem=recv.at[c, i if lands is None else lands],
                device_id=peer,
                device_id_type=pl.DeviceIdType.MESH,
            )

        def block(p, step):
            there = (spots[p] + step) % 4
            return pl.ds(pl.multiple_of(starts[p] + there * rows_of[p], 8), rows_of[p])

        def landing(p):
            return pl.ds(starts[p + 1], rows_of[p])

        def halve(p, part, got):
            return [
                copy(3 * p + d, part.at[block(p, d)], got.at[d - 1, landing(p)], along(axes[p], d, core))
                for d in (1, 2, 3)
            ]

        def mine(p, part, got):
            return (part[block(p, 0)] + got[0, landing(p)]) + (got[1, landing(p)] + got[2, landing(p)])

        at = [base + spots[0] * rows_of[0]]
        for p in (1, 2):
            at.append(at[-1] + spots[p] * rows_of[p])

        def spread(p):
            where = held.at[pl.ds(pl.multiple_of(at[p], 8), rows_of[p])]
            return [copy(14 + 3 * (2 - p) + d - 1, where, where, along(axes[p], d, core)) for d in (1, 2, 3)]

        beside = copy(7, part_c.at[block(2, 0)], last.at[core, 0, landing(2)], partner())
        finals, arrivals = [], []
        for d in (1, 2, 3):
            src, dst = part_c.at[block(2, d)], last.at[core, d, landing(2)]
            peer = along(axes[2], d, 1)
            finals.append(copy(7 + d, src, dst, peer, 10 + d - 3 * core))
            arrivals += [copy(7 + d, src, dst, peer, lands) for lands in (7 + d, 10 + d)]
        forward = copy(23, held.at[whole], held.at[whole], partner())

        def add_pair():
            part_a[whole] = sums[core, whole] + paired[whole]

        def add_a():
            part_b[landing(0)] = mine(0, part_a, got_a)

        def add_b():
            part_c[landing(1)] = mine(1, part_b, got_b)
            last[core, 0, landing(2)] = part_c[block(2, 0)]

        def solve():
            @pl.when(core == 1)
            def _():
                grad, hess = (
                    (last[k, 0, landing(2)] + last[k, 1, landing(2)])
                    + (last[k, 2, landing(2)] + last[k, 3, landing(2)])
                    for k in (0, 1)
                )
                where = pl.ds(pl.multiple_of(at[2], 8), rows_of[2])
                held[where] = -step_size * grad / (hess + ridge_term)

        first = copy(0, sums.at[1 - core, whole], paired.at[whole], partner())
        every = None
        a, b = halve(0, part_a, got_a), halve(1, part_b, got_b)
        self.steps = [
            ([([first], every, [first], every)], add_pair),
            ([(a, every, a, every)], add_a),
            ([(b, every, b, every)], add_b),
            ([(finals, every, arrivals, 1), ([beside], 0, [beside], 1)], solve),
            *(([(out, 1, out, 1)], None) for out in (spread(2), spread(1), spread(0))),
            ([([forward], 1, [forward], 0)], None),
        ]
        self.now = 0

    def start(self):
        for copies, sender, _, _ in self.steps[self.now][0]:
            on(sender, [copy.start for copy in copies])

    def advance(self):
        groups, then = self.steps[self.now]
        for _, _, copies, receiver in groups:
            on(receiver, [copy.wait_recv for copy in copies])
        if then is not None:
            then()
        self.now += 1
        if self.now < len(self.steps):
            self.start()

    def settle(self):
        for groups, _ in self.steps:
            for copies, sender, _, _ in groups:
                on(sender, [copy.wait_send for copy in copies])


def on(core, calls):
    def go():
        for call in calls:
            call()

    if core is None:
        go()
    else:
        pl.when(lax.axis_index(AXES[2]) == core)(go)


def gradients(predict, labels):
    exponent = jnp.exp(predict - jnp.max(predict, axis=0, keepdims=True))
    probability = exponent * (1.0 / jnp.sum(exponent, axis=0, keepdims=True))
    classes = lax.broadcasted_iota(jnp.int32, predict.shape, 0)
    gradient = jnp.where(classes == labels, probability - 1.0, probability)
    return gradient.astype(BF16), (probability * (1.0 - probability)).astype(BF16)


def leaf_slots(width):
    return [(lax.broadcasted_iota(jnp.int32, (16, width), 0) + 16 * j).astype(F32).astype(BF16) for j in range(4)]


def one_hot(ids, slots):
    shape = slots[0].shape
    one, zero = jnp.ones(shape, BF16), jnp.zeros(shape, BF16)
    ids = ids.astype(F32)
    rows = []
    for t in range(ids.shape[0]):
        held = jnp.broadcast_to(ids[t : t + 1], shape).astype(BF16)
        rows += [jnp.where(held == slot, one, zero) for slot in slots]
    return jnp.concatenate(rows, axis=0)


def half_sums(slot, ids, stacked, acc):
    rows = ids.shape[1] // 2
    slots = leaf_slots(TILE)
    trees = pl.ds(pl.multiple_of(slot // 2 * TREES_AT_ONCE, TREES_AT_ONCE), TREES_AT_ONCE)

    @pl.when(slot % 2 == 0)
    def _():
        acc[...] = jnp.zeros_like(acc)

    @pl.loop(0, rows, step=TILE * UNROLL)
    def _(first):
        total = None
        for u in range(UNROLL):
            cols = pl.ds(pl.multiple_of(slot % 2 * rows + first + u * TILE, TILE), TILE)
            matches = one_hot(ids[trees, cols], slots)
            part = lax.dot_general(
                matches, stacked[:, cols], (((1,), (1,)), ((), ())), preferred_element_type=F32
            )
            total = part if total is None else total + part
        acc[...] += total


def keep_sums(c, acc, sums):
    base = pl.multiple_of(c * WIDE, WIDE)
    sums[0, pl.ds(base, WIDE)] = acc[:, :LANES]
    for b in range(64):
        sums[1, pl.ds(base + turned(b) * 8, 8)] = acc[b * 8 : b * 8 + 8, LANES:]


def in_order(c, held, values):
    base = pl.multiple_of(c * WIDE, WIDE)
    for b in range(64):
        values[pl.ds(base + b * 8, 8)] = held[pl.ds(base + turned(b) * 8, 8)]


def class_major(values, first, table):
    for b in range(table.shape[1] // LANES):
        block = values[pl.ds(first + b * LANES, LANES)]
        table[:, b * LANES : (b + 1) * LANES] = block.T[: table.shape[0]].astype(BF16)


def plan():
    steps = lambda m: (1.5 + 0.4 * m, 3.5 + m, 3.5 + 0.3 * m, 3.5, 3.0, 3.0 + 0.3 * m, 3.0 + m, 1.5)
    ends = [sum(CHUNKS[: c + 1]) // TREES_AT_ONCE for c in range(len(CHUNKS))]
    newest = len(CHUNKS) - 1
    order, clock, due, now = [], 0.0, {}, {}
    waiting = []

    def advance(c):
        nonlocal clock
        clock = max(clock, due[c]) + 0.15
        now[c] += 1
        order.append(("advance", c))
        lengths = steps(CHUNKS[c] // TREES_AT_ONCE)
        if now[c] < len(lengths):
            due[c] = clock + lengths[now[c]]
        else:
            del due[c]
            waiting.append(c)

    for group in range(ends[-1]):
        for half in (0, 1):
            order.append(("sums", group, half))
            clock += HALF_US
            if half and group + 1 in ends:
                c = ends.index(group + 1)
                order.append(("start", c))
                now[c], due[c] = 0, clock + steps(CHUNKS[c] // TREES_AT_ONCE)[0]
            for c in sorted(due, key=due.get):
                if due[c] <= clock + EARLY_US:
                    advance(c)
    while newest in due:
        c = min(due, key=lambda c: due[c] - (0.3 if c == newest else 0.0))
        if waiting and due[c] - clock > APPLY_US * CHUNKS[waiting[0]] / 8 * 0.6:
            order.append(("apply", waiting.pop(0)))
            clock += APPLY_US * CHUNKS[order[-1][1]] / 8
        else:
            advance(c)
    order += [("advance", c) for c in due for _ in range(now[c], 8)]
    waiting += list(due)
    return order + [("apply", c) for c in waiting if c != newest]


def grow_kernel(predict, labels, ids, carried, values, *scratch):
    lbuf, ibuf, stacked, acc, table, sums, held = scratch[:7]
    bufs, send, recv, sems = scratch[7:-3], *scratch[-3:]
    classes, rows = predict.shape
    width = rows // PIECES
    greet()

    def read(i):
        cols = pl.ds(pl.multiple_of(i * width, width), width)
        return pltpu.make_async_copy(predict.at[:, cols], carried.at[:, cols], sems.at[i])

    labels_read = pltpu.make_async_copy(labels, lbuf, sems.at[PIECES])
    ids_read = pltpu.make_async_copy(ids, ibuf, sems.at[PIECES + 1])
    labels_read.start()
    for i in range(PIECES):
        read(i).start()
    ids_read.start()
    for k in (0, 1):
        stacked[k * LANES + 96 : (k + 1) * LANES] = jnp.zeros((LANES - 96, rows), BF16)
    labels_read.wait()

    @pl.loop(0, PIECES)
    def _(i):
        read(i).wait()

        @pl.loop(0, width, step=512)
        def _(first):
            cols = pl.ds(pl.multiple_of(i * width + first, 512), 512)
            gradient, hessian = gradients(carried[:, cols], lbuf[:, cols])
            stacked[:classes, cols] = gradient
            stacked[LANES : LANES + classes, cols] = hessian

    ids_read.wait()
    bases = [sum(CHUNKS[:c]) * LEAVES for c in range(len(CHUNKS))]
    chunks = [Exchange(c, CHUNKS[c], bases[c], sums, held, bufs, send, recv) for c in range(len(CHUNKS))]

    def apply(c):
        in_order(c, held, values)
        class_major(values, pl.multiple_of(c * WIDE, WIDE), table)
        slots = leaf_slots(TILE)
        trees = pl.ds(pl.multiple_of(c * TREES_AT_ONCE, TREES_AT_ONCE), TREES_AT_ONCE)

        @pl.loop(0, rows, step=APPLY * TILE)
        def _(first):
            for u in range(APPLY):
                cols = pl.ds(pl.multiple_of(first + u * TILE, TILE), TILE)
                update = jnp.dot(table[...], one_hot(ibuf[trees, cols], slots), preferred_element_type=F32)
                carried[:, cols] += update[:classes]

    def exchange(actions):
        for what, c in actions:
            getattr(chunks[c], what)()

    parts = [[]]
    for action in plan():
        if action[0] in ("sums", "apply"):
            parts.append([])
        else:
            parts[-1].append(action)
    halves = 2 * len(chunks)

    @pl.loop(0, halves)
    def _(slot):
        half_sums(slot, ibuf, stacked, acc)

        @pl.when(slot % 2 == 1)
        def _():
            keep_sums(slot // 2, acc, sums)

        for k in range(halves - 1):
            if parts[k + 1]:

                @pl.when(slot == k)
                def _():
                    if k == 1:
                        wait_for_all()
                    exchange(parts[k + 1])

    exchange(parts[halves])

    @pl.loop(0, len(chunks) - 1)
    def _(c):
        apply(c)
        for k in range(len(chunks) - 1):
            if parts[halves + 1 + k]:

                @pl.when(c == k)
                def _():
                    exchange(parts[halves + 1 + k])

    in_order(len(chunks) - 1, held, values)
    for chunk in chunks:
        chunk.settle()


def grow(predict, labels, ids):
    classes, rows = predict.shape
    leaves = ids.shape[0] * LEAVES
    k = len(CHUNKS)
    pinned = [pltpu.with_memory_space_constraint(a, pltpu.HBM) for a in (predict, labels, ids)]
    return pl.pallas_call(
        grow_kernel,
        out_shape=(jax.ShapeDtypeStruct(predict.shape, F32), jax.ShapeDtypeStruct((leaves, LANES), F32)),
        in_specs=[pl.BlockSpec(memory_space=pltpu.HBM)] * 3,
        out_specs=(pl.BlockSpec(memory_space=pltpu.VMEM), pl.BlockSpec(memory_space=pltpu.VMEM)),
        scratch_shapes=[
            pltpu.VMEM((1, rows), jnp.int32),
            pltpu.VMEM(ids.shape, jnp.int32),
            pltpu.VMEM((2 * LANES, rows), BF16),
            pltpu.VMEM((WIDE, 2 * LANES), F32),
            pltpu.VMEM((112, WIDE), BF16),
            pltpu.VMEM((2, leaves, LANES), F32),
            pltpu.VMEM((leaves, LANES), F32),
            pltpu.VMEM((leaves, LANES), F32),
            pltpu.VMEM((leaves, LANES), F32),
            pltpu.VMEM((3, leaves // 4, LANES), F32),
            pltpu.VMEM((leaves // 4, LANES), F32),
            pltpu.VMEM((3, leaves // 16, LANES), F32),
            pltpu.VMEM((leaves // 16, LANES), F32),
            pltpu.VMEM((2, 4, leaves // 64, LANES), F32),
            pltpu.SemaphoreType.DMA((k, COPIES)),
            pltpu.SemaphoreType.DMA((k, COPIES)),
            pltpu.SemaphoreType.DMA((PIECES + 2,)),
        ],
        compiler_params=pltpu.CompilerParams(
            collective_id=0, has_side_effects=True, vmem_limit_bytes=40 << 20
        ),
        name="grow",
    )(*pinned)


def finish_kernel(values, carried, ids, out, own, table, ibuf, obuf, sems, ids_sem):
    classes, rows = carried.shape
    width = rows // WRITES
    first_id = ids.shape[0] - CHUNKS[-1]
    ids_read = pltpu.make_async_copy(ids.at[pl.ds(first_id, CHUNKS[-1])], ibuf, ids_sem)
    ids_read.start()
    class_major(values, first_id * LEAVES, table)
    ids_read.wait()
    slots = leaf_slots(TILE)
    writes = []
    for i in range(WRITES):
        for u in range(width // TILE):
            cols = pl.ds(i * width + u * TILE, TILE)
            update = jnp.dot(table[...], one_hot(ibuf[:, cols], slots), preferred_element_type=F32)
            obuf[:, cols] = carried[:, cols] + update[:classes]
        cols = pl.ds(i * width, width)
        writes.append(pltpu.make_async_copy(obuf.at[:, cols], out.at[:, cols], sems.at[i]))
        writes[-1].start()
    own_width = own.shape[1]
    for b in range(own_width // LANES):
        first = pl.multiple_of(lax.axis_index("leaf") * own_width + b * LANES, LANES)
        own[:, b * LANES : (b + 1) * LANES] = values[pl.ds(first, LANES)].T[:classes]
    for write in writes:
        write.wait()


def finish(values, carried, ids):
    classes, rows = carried.shape
    own_width = values.shape[0] // lax.axis_size("leaf")
    return pl.pallas_call(
        finish_kernel,
        out_shape=(
            jax.ShapeDtypeStruct(carried.shape, F32),
            jax.ShapeDtypeStruct((classes, own_width), F32),
        ),
        in_specs=[
            pl.BlockSpec(memory_space=pltpu.VMEM),
            pl.BlockSpec(memory_space=pltpu.VMEM),
            pl.BlockSpec(memory_space=pl.ANY),
        ],
        out_specs=(pl.BlockSpec(memory_space=pl.ANY), pl.BlockSpec(memory_space=pltpu.VMEM)),
        scratch_shapes=[
            pltpu.VMEM((112, CHUNKS[-1] * LEAVES), BF16),
            pltpu.VMEM((CHUNKS[-1], rows), jnp.int32),
            pltpu.VMEM((classes, rows), F32),
            pltpu.SemaphoreType.DMA((WRITES,)),
            pltpu.SemaphoreType.DMA,
        ],
        compiler_params=pltpu.CompilerParams(vmem_limit_bytes=24 << 20),
        name="finish",
    )(values, carried, ids)


def shards(predict, labels, leaf_ids):
    carried, values = grow(predict, labels[None, :], leaf_ids)
    return finish(values, carried, leaf_ids)


def solution(mesh):
    finer = Mesh(mesh.devices.reshape(4, 4, 2, mesh.shape["leaf"]), AXES)
    in_specs = (P(None, AXES), P(AXES), P(None, AXES))
    out_specs = (P(None, AXES), P(None, "leaf"))
    return jax.shard_map(shards, mesh=finer, in_specs=in_specs, out_specs=out_specs, check_vma=False)
```

```python
import jax
import jax.numpy as jnp
from jax import lax
from jax.experimental import pallas as pl
from jax.experimental.pallas import tpu as pltpu
from jax.sharding import Mesh
from jax.sharding import PartitionSpec as P

F32, BF16 = jnp.float32, jnp.bfloat16
LEAVES = 64
AXES = ("dp_0", "dp_1", "dp_2", "leaf")
TREES_AT_ONCE = 8
WIDE = TREES_AT_ONCE * LEAVES
LANES = 128
CHUNKS = (8, 8, 8, 8)
COPIES = 16
TILE = 256
PIECES = 8
APPLY = 16
WRITES = 4
UNROLL = 16
HALF_US, APPLY_US, EARLY_US = 1.15, 1.9, 0.3

step_size = 0.5
ridge_term = 1.0


def turned(block):
    return (block // 4 % 4) * 16 + (block % 4) * 4 + block // 16


def places():
    y, x, core, z = (lax.axis_index(name) for name in AXES)
    return x, y, z, core


def picks(axis):
    return (1 - axis) * (2 - axis) // 2, axis * (2 - axis), axis * (axis - 1) // 2


def spot(axis):
    x, y, z, _ = places()
    px, py, pz = picks(axis)
    return px * x + py * y + pz * z


def along(axis, step, core):
    x, y, z, _ = places()
    px, py, pz = picks(axis)
    q = spot(axis)
    move = (q + step) % 4 - q
    return (y + py * move, x + px * move, core, z + pz * move)


def partner():
    x, y, z, core = places()
    return (y, x, 1 - core, z)


def everywhere(core):
    x, y, z, _ = places()
    moves = [(a, b, c) for a in range(4) for b in range(4) for c in range(4)][1:]
    moves.sort(key=lambda move: -sum(min(m, 4 - m) for m in move))
    return [((y + b) % 4, (x + a) % 4, core, (z + c) % 4) for a, b, c in moves]


def greeted():
    core = lax.axis_index(AXES[2])
    return everywhere(core) + [along(a, d, 1 - core) for a in range(3) for d in (1, 2, 3)] + [partner()]


def greet():
    barrier = pltpu.get_barrier_semaphore()
    for peer in greeted():
        pl.semaphore_signal(barrier, inc=1, device_id=peer, device_id_type=pl.DeviceIdType.MESH)


def wait_for_all():
    pl.semaphore_wait(pltpu.get_barrier_semaphore(), len(greeted()))


class Exchange:
    def __init__(self, c, trees, base, sums, held, bufs, send, recv):
        paired, part_a, got_a, part_b, got_b, part_c, last = bufs
        core = lax.axis_index(AXES[2])
        axes = [(c + core + p) % 3 for p in range(3)]
        spots = [spot(a) for a in axes]
        size = trees * LEAVES
        rows_of = [size // 4, size // 16, size // 64]
        whole = pl.ds(base, size)
        starts = [base, base // 4, base // 16, base // 64]

        def copy(i, src, dst, peer, lands=None):
            return pltpu.make_async_remote_copy(
                src_ref=src,
                dst_ref=dst,
                send_sem=send.at[c, i],
                recv_sem=recv.at[c, i if lands is None else lands],
                device_id=peer,
                device_id_type=pl.DeviceIdType.MESH,
            )

        def block(p, step):
            there = (spots[p] + step) % 4
            return pl.ds(pl.multiple_of(starts[p] + there * rows_of[p], 8), rows_of[p])

        def landing(p):
            return pl.ds(starts[p + 1], rows_of[p])

        def halve(p, part, got):
            return [
                copy(3 * p + d, part.at[block(p, d)], got.at[d - 1, landing(p)], along(axes[p], d, core))
                for d in (1, 2, 3)
            ]

        def mine(p, part, got):
            return (part[block(p, 0)] + got[0, landing(p)]) + (got[1, landing(p)] + got[2, landing(p)])

        first_row = base + sum(spots[p] * rows_of[p] for p in range(3))
        where = pl.ds(pl.multiple_of(first_row, 8), rows_of[2])

        beside = copy(7, part_c.at[block(2, 0)], last.at[core, 0, landing(2)], partner())
        finals, arrivals = [], []
        for d in (1, 2, 3):
            src, dst = part_c.at[block(2, d)], last.at[core, d, landing(2)]
            peer = along(axes[2], d, 1)
            finals.append(copy(7 + d, src, dst, peer, 10 + d - 3 * core))
            arrivals += [copy(7 + d, src, dst, peer, lands) for lands in (7 + d, 10 + d)]
        rounds = [copy(14, held.at[where], held.at[where], peer) for peer in everywhere(1)]
        others = pl.ds(base, size - rows_of[2])
        round_all = [copy(14, held.at[others], held.at[others], partner())]
        forward = copy(15, held.at[whole], held.at[whole], partner())

        def add_pair():
            part_a[whole] = sums[core, whole] + paired[whole]

        def add_a():
            part_b[landing(0)] = mine(0, part_a, got_a)

        def add_b():
            part_c[landing(1)] = mine(1, part_b, got_b)
            last[core, 0, landing(2)] = part_c[block(2, 0)]

        def solve():
            @pl.when(core == 1)
            def _():
                grad, hess = (
                    (last[k, 0, landing(2)] + last[k, 1, landing(2)])
                    + (last[k, 2, landing(2)] + last[k, 3, landing(2)])
                    for k in (0, 1)
                )
                held[where] = -step_size * grad / (hess + ridge_term)

        first = copy(0, sums.at[1 - core, whole], paired.at[whole], partner())
        every = None
        a, b = halve(0, part_a, got_a), halve(1, part_b, got_b)
        self.steps = [
            ([([first], every, [first], every)], add_pair),
            ([(a, every, a, every)], add_a),
            ([(b, every, b, every)], add_b),
            ([(finals, every, arrivals, 1), ([beside], 0, [beside], 1)], solve),
            ([(rounds, 1, round_all, 1)], None),
            ([([forward], 1, [forward], 0)], None),
        ]
        self.now = 0

    def start(self):
        for copies, sender, _, _ in self.steps[self.now][0]:
            on(sender, [copy.start for copy in copies])

    def advance(self):
        groups, then = self.steps[self.now]
        for _, _, copies, receiver in groups:
            on(receiver, [copy.wait_recv for copy in copies])
        if then is not None:
            then()
        self.now += 1
        if self.now < len(self.steps):
            self.start()

    def settle(self):
        for groups, _ in self.steps:
            for copies, sender, arrivals, _ in groups:
                out = arrivals if len(arrivals) == 1 else copies
                on(sender, [copy.wait_send for copy in out])


def on(core, calls):
    def go():
        for call in calls:
            call()

    if core is None:
        go()
    else:
        pl.when(lax.axis_index(AXES[2]) == core)(go)


def gradients(predict, labels):
    exponent = jnp.exp(predict - jnp.max(predict, axis=0, keepdims=True))
    probability = exponent * (1.0 / jnp.sum(exponent, axis=0, keepdims=True))
    classes = lax.broadcasted_iota(jnp.int32, predict.shape, 0)
    gradient = jnp.where(classes == labels, probability - 1.0, probability)
    return gradient.astype(BF16), (probability * (1.0 - probability)).astype(BF16)


def leaf_slots(width):
    return [(lax.broadcasted_iota(jnp.int32, (16, width), 0) + 16 * j).astype(F32).astype(BF16) for j in range(4)]


def one_hot(ids, slots):
    shape = slots[0].shape
    one, zero = jnp.ones(shape, BF16), jnp.zeros(shape, BF16)
    ids = ids.astype(F32)
    rows = []
    for t in range(ids.shape[0]):
        held = jnp.broadcast_to(ids[t : t + 1], shape).astype(BF16)
        rows += [jnp.where(held == slot, one, zero) for slot in slots]
    return jnp.concatenate(rows, axis=0)


def half_sums(slot, ids, stacked, acc):
    rows = ids.shape[1] // 2
    slots = leaf_slots(TILE)
    trees = pl.ds(pl.multiple_of(slot // 2 * TREES_AT_ONCE, TREES_AT_ONCE), TREES_AT_ONCE)

    @pl.when(slot % 2 == 0)
    def _():
        acc[...] = jnp.zeros_like(acc)

    @pl.loop(0, rows, step=TILE * UNROLL)
    def _(first):
        total = None
        for u in range(UNROLL):
            cols = pl.ds(pl.multiple_of(slot % 2 * rows + first + u * TILE, TILE), TILE)
            matches = one_hot(ids[trees, cols], slots)
            part = lax.dot_general(
                matches, stacked[:, cols], (((1,), (1,)), ((), ())), preferred_element_type=F32
            )
            total = part if total is None else total + part
        acc[...] += total


def keep_sums(c, acc, sums):
    base = pl.multiple_of(c * WIDE, WIDE)
    sums[0, pl.ds(base, WIDE)] = acc[:, :LANES]
    for b in range(64):
        sums[1, pl.ds(base + turned(b) * 8, 8)] = acc[b * 8 : b * 8 + 8, LANES:]


def in_order(c, held, values):
    base = pl.multiple_of(c * WIDE, WIDE)
    for b in range(64):
        values[pl.ds(base + b * 8, 8)] = held[pl.ds(base + turned(b) * 8, 8)]


def class_major(values, first, table):
    for b in range(table.shape[1] // LANES):
        block = values[pl.ds(first + b * LANES, LANES)]
        table[:, b * LANES : (b + 1) * LANES] = block.T[: table.shape[0]].astype(BF16)


def plan():
    steps = lambda m: (1.5 + 0.4 * m, 3.5 + m, 3.5 + 0.3 * m, 3.5, 8.0 + 0.5 * m, 1.5)
    ends = [sum(CHUNKS[: c + 1]) // TREES_AT_ONCE for c in range(len(CHUNKS))]
    newest = len(CHUNKS) - 1
    order, clock, due, now = [], 0.0, {}, {}
    waiting = []

    def advance(c):
        nonlocal clock
        clock = max(clock, due[c]) + 0.15
        now[c] += 1
        order.append(("advance", c))
        lengths = steps(CHUNKS[c] // TREES_AT_ONCE)
        if now[c] < len(lengths):
            due[c] = clock + lengths[now[c]]
        else:
            del due[c]
            waiting.append(c)

    for group in range(ends[-1]):
        for half in (0, 1):
            order.append(("sums", group, half))
            clock += HALF_US
            if half and group + 1 in ends:
                c = ends.index(group + 1)
                order.append(("start", c))
                now[c], due[c] = 0, clock + steps(CHUNKS[c] // TREES_AT_ONCE)[0]
            for c in sorted(due, key=due.get):
                if due[c] <= clock + EARLY_US:
                    advance(c)
    while newest in due:
        c = min(due, key=lambda c: due[c] - (0.3 if c == newest else 0.0))
        if waiting and due[c] - clock > APPLY_US * CHUNKS[waiting[0]] / 8 * 0.6:
            order.append(("apply", waiting.pop(0)))
            clock += APPLY_US * CHUNKS[order[-1][1]] / 8
        else:
            advance(c)
    order += [("advance", c) for c in due for _ in range(now[c], 6)]
    waiting += list(due)
    return order + [("apply", c) for c in waiting if c != newest]


def grow_kernel(predict, labels, ids, carried, values, *scratch):
    lbuf, ibuf, stacked, acc, table, sums, held = scratch[:7]
    bufs, send, recv, sems = scratch[7:-3], *scratch[-3:]
    classes, rows = predict.shape
    width = rows // PIECES
    greet()

    def read(i):
        cols = pl.ds(pl.multiple_of(i * width, width), width)
        return pltpu.make_async_copy(predict.at[:, cols], carried.at[:, cols], sems.at[i])

    labels_read = pltpu.make_async_copy(labels, lbuf, sems.at[PIECES])
    ids_read = pltpu.make_async_copy(ids, ibuf, sems.at[PIECES + 1])
    labels_read.start()
    for i in range(PIECES):
        read(i).start()
    ids_read.start()
    for k in (0, 1):
        stacked[k * LANES + 96 : (k + 1) * LANES] = jnp.zeros((LANES - 96, rows), BF16)
    labels_read.wait()

    @pl.loop(0, PIECES)
    def _(i):
        read(i).wait()

        @pl.loop(0, width, step=512)
        def _(first):
            cols = pl.ds(pl.multiple_of(i * width + first, 512), 512)
            gradient, hessian = gradients(carried[:, cols], lbuf[:, cols])
            stacked[:classes, cols] = gradient
            stacked[LANES : LANES + classes, cols] = hessian

    ids_read.wait()
    bases = [sum(CHUNKS[:c]) * LEAVES for c in range(len(CHUNKS))]
    chunks = [Exchange(c, CHUNKS[c], bases[c], sums, held, bufs, send, recv) for c in range(len(CHUNKS))]

    def apply(c):
        in_order(c, held, values)
        class_major(values, pl.multiple_of(c * WIDE, WIDE), table)
        slots = leaf_slots(TILE)
        trees = pl.ds(pl.multiple_of(c * TREES_AT_ONCE, TREES_AT_ONCE), TREES_AT_ONCE)

        @pl.loop(0, rows, step=APPLY * TILE)
        def _(first):
            for u in range(APPLY):
                cols = pl.ds(pl.multiple_of(first + u * TILE, TILE), TILE)
                update = jnp.dot(table[...], one_hot(ibuf[trees, cols], slots), preferred_element_type=F32)
                carried[:, cols] += update[:classes]

    def exchange(actions):
        for what, c in actions:
            getattr(chunks[c], what)()

    parts = [[]]
    for action in plan():
        if action[0] in ("sums", "apply"):
            parts.append([])
        else:
            parts[-1].append(action)
    halves = 2 * len(chunks)

    @pl.loop(0, halves)
    def _(slot):
        half_sums(slot, ibuf, stacked, acc)

        @pl.when(slot % 2 == 1)
        def _():
            keep_sums(slot // 2, acc, sums)

        for k in range(halves - 1):
            if parts[k + 1]:

                @pl.when(slot == k)
                def _():
                    if k == 1:
                        wait_for_all()
                    exchange(parts[k + 1])

    exchange(parts[halves])

    @pl.loop(0, len(chunks) - 1)
    def _(c):
        apply(c)
        for k in range(len(chunks) - 1):
            if parts[halves + 1 + k]:

                @pl.when(c == k)
                def _():
                    exchange(parts[halves + 1 + k])

    in_order(len(chunks) - 1, held, values)
    for chunk in chunks:
        chunk.settle()


def grow(predict, labels, ids):
    classes, rows = predict.shape
    leaves = ids.shape[0] * LEAVES
    k = len(CHUNKS)
    pinned = [pltpu.with_memory_space_constraint(a, pltpu.HBM) for a in (predict, labels, ids)]
    return pl.pallas_call(
        grow_kernel,
        out_shape=(jax.ShapeDtypeStruct(predict.shape, F32), jax.ShapeDtypeStruct((leaves, LANES), F32)),
        in_specs=[pl.BlockSpec(memory_space=pltpu.HBM)] * 3,
        out_specs=(pl.BlockSpec(memory_space=pltpu.VMEM), pl.BlockSpec(memory_space=pltpu.VMEM)),
        scratch_shapes=[
            pltpu.VMEM((1, rows), jnp.int32),
            pltpu.VMEM(ids.shape, jnp.int32),
            pltpu.VMEM((2 * LANES, rows), BF16),
            pltpu.VMEM((WIDE, 2 * LANES), F32),
            pltpu.VMEM((112, WIDE), BF16),
            pltpu.VMEM((2, leaves, LANES), F32),
            pltpu.VMEM((leaves, LANES), F32),
            pltpu.VMEM((leaves, LANES), F32),
            pltpu.VMEM((leaves, LANES), F32),
            pltpu.VMEM((3, leaves // 4, LANES), F32),
            pltpu.VMEM((leaves // 4, LANES), F32),
            pltpu.VMEM((3, leaves // 16, LANES), F32),
            pltpu.VMEM((leaves // 16, LANES), F32),
            pltpu.VMEM((2, 4, leaves // 64, LANES), F32),
            pltpu.SemaphoreType.DMA((k, COPIES)),
            pltpu.SemaphoreType.DMA((k, COPIES)),
            pltpu.SemaphoreType.DMA((PIECES + 2,)),
        ],
        compiler_params=pltpu.CompilerParams(
            collective_id=0, has_side_effects=True, vmem_limit_bytes=40 << 20
        ),
        name="grow",
    )(*pinned)


def finish_kernel(values, carried, ids, out, own, table, ibuf, obuf, sems, ids_sem):
    classes, rows = carried.shape
    width = rows // WRITES
    first_id = ids.shape[0] - CHUNKS[-1]
    ids_read = pltpu.make_async_copy(ids.at[pl.ds(first_id, CHUNKS[-1])], ibuf, ids_sem)
    ids_read.start()
    class_major(values, first_id * LEAVES, table)
    ids_read.wait()
    slots = leaf_slots(TILE)
    writes = []
    for i in range(WRITES):
        for u in range(width // TILE):
            cols = pl.ds(i * width + u * TILE, TILE)
            update = jnp.dot(table[...], one_hot(ibuf[:, cols], slots), preferred_element_type=F32)
            obuf[:, cols] = carried[:, cols] + update[:classes]
        cols = pl.ds(i * width, width)
        writes.append(pltpu.make_async_copy(obuf.at[:, cols], out.at[:, cols], sems.at[i]))
        writes[-1].start()
    own_width = own.shape[1]
    for b in range(own_width // LANES):
        first = pl.multiple_of(lax.axis_index("leaf") * own_width + b * LANES, LANES)
        own[:, b * LANES : (b + 1) * LANES] = values[pl.ds(first, LANES)].T[:classes]
    for write in writes:
        write.wait()


def finish(values, carried, ids):
    classes, rows = carried.shape
    own_width = values.shape[0] // lax.axis_size("leaf")
    return pl.pallas_call(
        finish_kernel,
        out_shape=(
            jax.ShapeDtypeStruct(carried.shape, F32),
            jax.ShapeDtypeStruct((classes, own_width), F32),
        ),
        in_specs=[
            pl.BlockSpec(memory_space=pltpu.VMEM),
            pl.BlockSpec(memory_space=pltpu.VMEM),
            pl.BlockSpec(memory_space=pl.ANY),
        ],
        out_specs=(pl.BlockSpec(memory_space=pl.ANY), pl.BlockSpec(memory_space=pltpu.VMEM)),
        scratch_shapes=[
            pltpu.VMEM((112, CHUNKS[-1] * LEAVES), BF16),
            pltpu.VMEM((CHUNKS[-1], rows), jnp.int32),
            pltpu.VMEM((classes, rows), F32),
            pltpu.SemaphoreType.DMA((WRITES,)),
            pltpu.SemaphoreType.DMA,
        ],
        compiler_params=pltpu.CompilerParams(vmem_limit_bytes=24 << 20),
        name="finish",
    )(values, carried, ids)


def shards(predict, labels, leaf_ids):
    carried, values = grow(predict, labels[None, :], leaf_ids)
    return finish(values, carried, leaf_ids)


def solution(mesh):
    finer = Mesh(mesh.devices.reshape(4, 4, 2, mesh.shape["leaf"]), AXES)
    in_specs = (P(None, AXES), P(AXES), P(None, AXES))
    out_specs = (P(None, AXES), P(None, "leaf"))
    return jax.shard_map(shards, mesh=finer, in_specs=in_specs, out_specs=out_specs, check_vma=False)
```

```python
import jax
import jax.numpy as jnp
from jax import lax
from jax.experimental import pallas as pl
from jax.experimental.pallas import tpu as pltpu
from jax.sharding import Mesh
from jax.sharding import PartitionSpec as P

F32, BF16 = jnp.float32, jnp.bfloat16
LEAVES = 64
AXES = ("dp_0", "dp_1", "dp_2", "leaf")
TREES_AT_ONCE = 8
WIDE = TREES_AT_ONCE * LEAVES
LANES = 128
CHUNKS = (8, 8, 8, 8)
COPIES = 6
TILE = 256
PIECES = 8
APPLY = 16
WRITES = 4
UNROLL = 16
HALF_US, APPLY_US, EARLY_US = 1.15, 1.9, 0.3

step_size = 0.5
ridge_term = 1.0


def places():
    y, x, core, z = (lax.axis_index(name) for name in AXES)
    return x, y, z, core


def partner():
    x, y, z, core = places()
    return (y, x, 1 - core, z)


def moves():
    found = [(a, b, c) for a in range(4) for b in range(4) for c in range(4)][1:]
    return sorted(found, key=lambda move: -sum(min(m, 4 - m) for m in move))


def chip_at(move, core):
    x, y, z, _ = places()
    a, b, c = ((at + m) % 4 for at, m in zip((x, y, z), move))
    return (b, a, core, c), a * 16 + b * 4 + c


def greet():
    barrier = pltpu.get_barrier_semaphore()

    def call(core):
        peers = [partner()] if core == 1 else []
        for peer in peers + [chip_at(move, core)[0] for move in moves()]:
            pl.semaphore_signal(barrier, inc=1, device_id=peer, device_id_type=pl.DeviceIdType.MESH)

    call(1)

    @pl.when(lax.axis_index(AXES[2]) == 1)
    def _():
        call(0)


def wait_for_all():
    pl.semaphore_wait(pltpu.get_barrier_semaphore(), 64 + 63 * lax.axis_index(AXES[2]))


class Exchange:
    def __init__(self, c, trees, base, sums, held, bufs, send, recv):
        paired, summed, last = bufs
        x, y, z, core = places()
        size = trees * LEAVES
        rows = size // 64
        whole = pl.ds(base, size)

        def copy(i, src, dst, peer, lands=None):
            return pltpu.make_async_remote_copy(
                src_ref=src,
                dst_ref=dst,
                send_sem=send.at[c, i],
                recv_sem=recv.at[c, i if lands is None else lands],
                device_id=peer,
                device_id_type=pl.DeviceIdType.MESH,
            )

        def block(chip):
            return pl.ds(pl.multiple_of(base + chip * rows, 8), rows)

        own = block(x * 16 + y * 4 + z)
        pieces, rounds = [], []
        for n, move in enumerate(moves()):
            peer, chip = chip_at(move, 1)
            pieces.append(copy(1, summed.at[block(chip)], last.at[c, core, n], peer, 2 - core))
            rounds.append(copy(4, held.at[own], held.at[own], peer))
        others = pl.ds(0, 63)
        arrived = [copy(1, last.at[c, k, others], last.at[c, k, others], partner(), 2 - k) for k in (0, 1)]
        beside = copy(3, summed.at[own], last.at[c, 0, 63], partner())
        rest = held.at[pl.ds(base, size - rows)]
        first = copy(0, sums.at[1 - core, whole], paired.at[whole], partner())
        forward = copy(5, held.at[whole], held.at[whole], partner())

        def add_pair():
            summed[whole] = sums[core, whole] + paired[whole]

        def solve():
            @pl.when(core == 1)
            def _():
                last[c, 1, 63] = summed[own]
                grad, hess = (jnp.sum(last[c, k], axis=0) for k in (0, 1))
                held[own] = -step_size * grad / (hess + ridge_term)

        self.steps = [
            ([([first], None, [first], None)], add_pair),
            ([(pieces, None, arrived, 1), ([beside], 0, [beside], 1)], solve),
            ([(rounds, 1, [copy(4, rest, rest, partner())], 1)], None),
            ([([forward], 1, [forward], 0)], None),
        ]
        self.now = 0

    def start(self):
        for copies, sender, _, _ in self.steps[self.now][0]:
            on(sender, [copy.start for copy in copies])

    def advance(self):
        groups, then = self.steps[self.now]
        for _, _, copies, receiver in groups:
            on(receiver, [copy.wait_recv for copy in copies])
        if then is not None:
            then()
        self.now += 1
        if self.now < len(self.steps):
            self.start()

    def settle(self):
        for groups, _ in self.steps:
            for copies, sender, arrivals, _ in groups:
                on(sender, [arrivals[0].wait_send])


def on(core, calls):
    def go():
        for call in calls:
            call()

    if core is None:
        go()
    else:
        pl.when(lax.axis_index(AXES[2]) == core)(go)


def gradients(predict, labels):
    exponent = jnp.exp(predict - jnp.max(predict, axis=0, keepdims=True))
    probability = exponent * (1.0 / jnp.sum(exponent, axis=0, keepdims=True))
    classes = lax.broadcasted_iota(jnp.int32, predict.shape, 0)
    gradient = jnp.where(classes == labels, probability - 1.0, probability)
    return gradient.astype(BF16), (probability * (1.0 - probability)).astype(BF16)


def leaf_slots(width):
    return [(lax.broadcasted_iota(jnp.int32, (16, width), 0) + 16 * j).astype(F32).astype(BF16) for j in range(4)]


def one_hot(ids, slots):
    shape = slots[0].shape
    one, zero = jnp.ones(shape, BF16), jnp.zeros(shape, BF16)
    ids = ids.astype(F32)
    rows = []
    for t in range(ids.shape[0]):
        held = jnp.broadcast_to(ids[t : t + 1], shape).astype(BF16)
        rows += [jnp.where(held == slot, one, zero) for slot in slots]
    return jnp.concatenate(rows, axis=0)


def half_sums(slot, ids, stacked, acc):
    rows = ids.shape[1] // 2
    slots = leaf_slots(TILE)
    trees = pl.ds(pl.multiple_of(slot // 2 * TREES_AT_ONCE, TREES_AT_ONCE), TREES_AT_ONCE)

    @pl.when(slot % 2 == 0)
    def _():
        acc[...] = jnp.zeros_like(acc)

    @pl.loop(0, rows, step=TILE * UNROLL)
    def _(first):
        total = None
        for u in range(UNROLL):
            cols = pl.ds(pl.multiple_of(slot % 2 * rows + first + u * TILE, TILE), TILE)
            matches = one_hot(ids[trees, cols], slots)
            part = lax.dot_general(
                matches, stacked[:, cols], (((1,), (1,)), ((), ())), preferred_element_type=F32
            )
            total = part if total is None else total + part
        acc[...] += total


def keep_sums(c, acc, sums):
    base = pl.multiple_of(c * WIDE, WIDE)
    sums[0, pl.ds(base, WIDE)] = acc[:, :LANES]
    sums[1, pl.ds(base, WIDE)] = acc[:, LANES:]


def class_major(values, first, table):
    for b in range(table.shape[1] // LANES):
        block = values[pl.ds(first + b * LANES, LANES)]
        table[:, b * LANES : (b + 1) * LANES] = block.T[: table.shape[0]].astype(BF16)


def plan():
    steps = lambda m: (1.5 + 0.4 * m, 8.0 + m, 8.0 + 0.5 * m, 1.5)
    ends = [sum(CHUNKS[: c + 1]) // TREES_AT_ONCE for c in range(len(CHUNKS))]
    newest = len(CHUNKS) - 1
    order, clock, due, now = [], 0.0, {}, {}
    waiting = []

    def advance(c):
        nonlocal clock
        clock = max(clock, due[c]) + 0.15
        now[c] += 1
        order.append(("advance", c))
        lengths = steps(CHUNKS[c] // TREES_AT_ONCE)
        if now[c] < len(lengths):
            due[c] = clock + lengths[now[c]]
        else:
            del due[c]
            waiting.append(c)

    for group in range(ends[-1]):
        for half in (0, 1):
            order.append(("sums", group, half))
            clock += HALF_US
            if half and group + 1 in ends:
                c = ends.index(group + 1)
                order.append(("start", c))
                now[c], due[c] = 0, clock + steps(CHUNKS[c] // TREES_AT_ONCE)[0]
            for c in sorted(due, key=due.get):
                if due[c] <= clock + EARLY_US:
                    advance(c)
    while newest in due:
        c = min(due, key=lambda c: due[c] - (0.3 if c == newest else 0.0))
        if waiting and due[c] - clock > APPLY_US * CHUNKS[waiting[0]] / 8 * 0.6:
            order.append(("apply", waiting.pop(0)))
            clock += APPLY_US * CHUNKS[order[-1][1]] / 8
        else:
            advance(c)
    order += [("advance", c) for c in due for _ in range(now[c], 4)]
    waiting += list(due)
    return order + [("apply", c) for c in waiting if c != newest]


def grow_kernel(predict, labels, ids, carried, values, *scratch):
    lbuf, ibuf, stacked, acc, table, sums, held = scratch[:7]
    bufs, send, recv, sems = scratch[7:-3], *scratch[-3:]
    classes, rows = predict.shape
    width = rows // PIECES
    greet()

    def read(i):
        cols = pl.ds(pl.multiple_of(i * width, width), width)
        return pltpu.make_async_copy(predict.at[:, cols], carried.at[:, cols], sems.at[i])

    labels_read = pltpu.make_async_copy(labels, lbuf, sems.at[PIECES])
    ids_read = pltpu.make_async_copy(ids, ibuf, sems.at[PIECES + 1])
    labels_read.start()
    for i in range(PIECES):
        read(i).start()
    ids_read.start()
    for k in (0, 1):
        stacked[k * LANES + 96 : (k + 1) * LANES] = jnp.zeros((LANES - 96, rows), BF16)
    labels_read.wait()

    @pl.loop(0, PIECES)
    def _(i):
        read(i).wait()

        @pl.loop(0, width, step=512)
        def _(first):
            cols = pl.ds(pl.multiple_of(i * width + first, 512), 512)
            gradient, hessian = gradients(carried[:, cols], lbuf[:, cols])
            stacked[:classes, cols] = gradient
            stacked[LANES : LANES + classes, cols] = hessian

    ids_read.wait()
    bases = [sum(CHUNKS[:c]) * LEAVES for c in range(len(CHUNKS))]
    chunks = [Exchange(c, CHUNKS[c], bases[c], sums, held, bufs, send, recv) for c in range(len(CHUNKS))]

    def apply(c):
        class_major(held, pl.multiple_of(c * WIDE, WIDE), table)
        slots = leaf_slots(TILE)
        trees = pl.ds(pl.multiple_of(c * TREES_AT_ONCE, TREES_AT_ONCE), TREES_AT_ONCE)

        @pl.loop(0, rows, step=APPLY * TILE)
        def _(first):
            for u in range(APPLY):
                cols = pl.ds(pl.multiple_of(first + u * TILE, TILE), TILE)
                update = jnp.dot(table[...], one_hot(ibuf[trees, cols], slots), preferred_element_type=F32)
                carried[:, cols] += update[:classes]

    def exchange(actions):
        for what, c in actions:
            getattr(chunks[c], what)()

    parts = [[]]
    for action in plan():
        if action[0] in ("sums", "apply"):
            parts.append([])
        else:
            parts[-1].append(action)
    halves = 2 * len(chunks)

    @pl.loop(0, halves)
    def _(slot):
        half_sums(slot, ibuf, stacked, acc)

        @pl.when(slot % 2 == 1)
        def _():
            keep_sums(slot // 2, acc, sums)

        for k in range(halves - 1):
            if parts[k + 1]:

                @pl.when(slot == k)
                def _():
                    if k == 1:
                        wait_for_all()
                    exchange(parts[k + 1])

    exchange(parts[halves])

    @pl.loop(0, len(chunks) - 1)
    def _(c):
        apply(c)
        for k in range(len(chunks) - 1):
            if parts[halves + 1 + k]:

                @pl.when(c == k)
                def _():
                    exchange(parts[halves + 1 + k])

    values[...] = held[...]
    for chunk in chunks:
        chunk.settle()


def grow(predict, labels, ids):
    classes, rows = predict.shape
    leaves = ids.shape[0] * LEAVES
    k = len(CHUNKS)
    pinned = [pltpu.with_memory_space_constraint(a, pltpu.HBM) for a in (predict, labels, ids)]
    return pl.pallas_call(
        grow_kernel,
        out_shape=(jax.ShapeDtypeStruct(predict.shape, F32), jax.ShapeDtypeStruct((leaves, LANES), F32)),
        in_specs=[pl.BlockSpec(memory_space=pltpu.HBM)] * 3,
        out_specs=(pl.BlockSpec(memory_space=pltpu.VMEM), pl.BlockSpec(memory_space=pltpu.VMEM)),
        scratch_shapes=[
            pltpu.VMEM((1, rows), jnp.int32),
            pltpu.VMEM(ids.shape, jnp.int32),
            pltpu.VMEM((2 * LANES, rows), BF16),
            pltpu.VMEM((WIDE, 2 * LANES), F32),
            pltpu.VMEM((112, WIDE), BF16),
            pltpu.VMEM((2, leaves, LANES), F32),
            pltpu.VMEM((leaves, LANES), F32),
            pltpu.VMEM((leaves, LANES), F32),
            pltpu.VMEM((leaves, LANES), F32),
            pltpu.VMEM((k, 2, 64, leaves // k // 64, LANES), F32),
            pltpu.SemaphoreType.DMA((k, COPIES)),
            pltpu.SemaphoreType.DMA((k, COPIES)),
            pltpu.SemaphoreType.DMA((PIECES + 2,)),
        ],
        compiler_params=pltpu.CompilerParams(
            collective_id=0, has_side_effects=True, vmem_limit_bytes=40 << 20
        ),
        name="grow",
    )(*pinned)


def finish_kernel(values, carried, ids, out, own, table, ibuf, obuf, sems, ids_sem):
    classes, rows = carried.shape
    width = rows // WRITES
    first_id = ids.shape[0] - CHUNKS[-1]
    ids_read = pltpu.make_async_copy(ids.at[pl.ds(first_id, CHUNKS[-1])], ibuf, ids_sem)
    ids_read.start()
    class_major(values, first_id * LEAVES, table)
    ids_read.wait()
    slots = leaf_slots(TILE)
    writes = []
    for i in range(WRITES):
        for u in range(width // TILE):
            cols = pl.ds(i * width + u * TILE, TILE)
            update = jnp.dot(table[...], one_hot(ibuf[:, cols], slots), preferred_element_type=F32)
            obuf[:, cols] = carried[:, cols] + update[:classes]
        cols = pl.ds(i * width, width)
        writes.append(pltpu.make_async_copy(obuf.at[:, cols], out.at[:, cols], sems.at[i]))
        writes[-1].start()
    own_width = own.shape[1]
    for b in range(own_width // LANES):
        first = pl.multiple_of(lax.axis_index("leaf") * own_width + b * LANES, LANES)
        own[:, b * LANES : (b + 1) * LANES] = values[pl.ds(first, LANES)].T[:classes]
    for write in writes:
        write.wait()


def finish(values, carried, ids):
    classes, rows = carried.shape
    own_width = values.shape[0] // lax.axis_size("leaf")
    return pl.pallas_call(
        finish_kernel,
        out_shape=(
            jax.ShapeDtypeStruct(carried.shape, F32),
            jax.ShapeDtypeStruct((classes, own_width), F32),
        ),
        in_specs=[
            pl.BlockSpec(memory_space=pltpu.VMEM),
            pl.BlockSpec(memory_space=pltpu.VMEM),
            pl.BlockSpec(memory_space=pl.ANY),
        ],
        out_specs=(pl.BlockSpec(memory_space=pl.ANY), pl.BlockSpec(memory_space=pltpu.VMEM)),
        scratch_shapes=[
            pltpu.VMEM((112, CHUNKS[-1] * LEAVES), BF16),
            pltpu.VMEM((CHUNKS[-1], rows), jnp.int32),
            pltpu.VMEM((classes, rows), F32),
            pltpu.SemaphoreType.DMA((WRITES,)),
            pltpu.SemaphoreType.DMA,
        ],
        compiler_params=pltpu.CompilerParams(vmem_limit_bytes=24 << 20),
        name="finish",
    )(values, carried, ids)


def shards(predict, labels, leaf_ids):
    carried, values = grow(predict, labels[None, :], leaf_ids)
    return finish(values, carried, leaf_ids)


def solution(mesh):
    finer = Mesh(mesh.devices.reshape(4, 4, 2, mesh.shape["leaf"]), AXES)
    in_specs = (P(None, AXES), P(AXES), P(None, AXES))
    out_specs = (P(None, AXES), P(None, "leaf"))
    return jax.shard_map(shards, mesh=finer, in_specs=in_specs, out_specs=out_specs, check_vma=False)
```

```python
import jax
import jax.numpy as jnp
from jax import lax
from jax.experimental import pallas as pl
from jax.experimental.pallas import tpu as pltpu
from jax.sharding import Mesh
from jax.sharding import PartitionSpec as P

F32, BF16 = jnp.float32, jnp.bfloat16
LEAVES = 64
AXES = ("dp_0", "dp_1", "dp_2", "leaf")
TREES_AT_ONCE = 8
WIDE = TREES_AT_ONCE * LEAVES
LANES = 128
CHUNKS = (8, 8, 8, 8)
COPIES = 6
TILE = 256
PIECES = 8
APPLY = 16
WRITES = 4
UNROLL = 16
SOFTMAX = 1024
HALF_US, APPLY_US, EARLY_US = 1.15, 1.9, 1.2

step_size = 0.5
ridge_term = 1.0


def places():
    y, x, core, z = (lax.axis_index(name) for name in AXES)
    return x, y, z, core


def partner():
    x, y, z, core = places()
    return (y, x, 1 - core, z)


def moves():
    found = [(a, b, c) for a in range(4) for b in range(4) for c in range(4)][1:]
    return sorted(found, key=lambda move: -sum(min(m, 4 - m) for m in move))


def chip_at(move, core):
    x, y, z, _ = places()
    a, b, c = ((at + m) % 4 for at, m in zip((x, y, z), move))
    return (b, a, core, c), a * 16 + b * 4 + c


def greet():
    barrier = pltpu.get_barrier_semaphore()

    def call(core):
        peers = [partner()] if core == 1 else []
        for peer in peers + [chip_at(move, core)[0] for move in moves()]:
            pl.semaphore_signal(barrier, inc=1, device_id=peer, device_id_type=pl.DeviceIdType.MESH)

    call(1)

    @pl.when(lax.axis_index(AXES[2]) == 1)
    def _():
        call(0)


def wait_for_all():
    pl.semaphore_wait(pltpu.get_barrier_semaphore(), 64 + 63 * lax.axis_index(AXES[2]))


class Exchange:
    def __init__(self, c, trees, base, sums, held, bufs, send, recv):
        paired, summed, last = bufs
        x, y, z, core = places()
        size = trees * LEAVES
        rows = size // 64
        whole = pl.ds(base, size)

        def copy(i, src, dst, peer, lands=None):
            return pltpu.make_async_remote_copy(
                src_ref=src,
                dst_ref=dst,
                send_sem=send.at[c, i],
                recv_sem=recv.at[c, i if lands is None else lands],
                device_id=peer,
                device_id_type=pl.DeviceIdType.MESH,
            )

        def block(chip):
            return pl.ds(pl.multiple_of(base + chip * rows, 8), rows)

        own = block(x * 16 + y * 4 + z)
        pieces, rounds = [], []
        for n, move in enumerate(moves()):
            peer, chip = chip_at(move, 1)
            pieces.append(copy(1, summed.at[block(chip)], last.at[c, core, n], peer, 2 - core))
            rounds.append(copy(4, held.at[own], held.at[own], peer))
        others = pl.ds(0, 63)
        arrived = [copy(1, last.at[c, k, others], last.at[c, k, others], partner(), 2 - k) for k in (0, 1)]
        beside = copy(3, summed.at[own], last.at[c, 0, 63], partner())
        rest = held.at[pl.ds(base, size - rows)]
        first = copy(0, sums.at[1 - core, whole], paired.at[whole], partner())
        forward = copy(5, held.at[whole], held.at[whole], partner())

        def add_pair():
            summed[whole] = sums[core, whole] + paired[whole]

        def solve():
            @pl.when(core == 1)
            def _():
                last[c, 1, 63] = summed[own]
                grad, hess = (jnp.sum(last[c, k], axis=0) for k in (0, 1))
                held[own] = -step_size * grad / (hess + ridge_term)

        self.steps = [
            ([([first], None, [first], None)], add_pair),
            ([(pieces, None, arrived, 1), ([beside], 0, [beside], 1)], solve),
            ([(rounds, 1, [copy(4, rest, rest, partner())], 1)], None),
            ([([forward], 1, [forward], 0)], None),
        ]
        self.now = 0

    def start(self):
        for copies, sender, _, _ in self.steps[self.now][0]:
            on(sender, [copy.start for copy in copies])

    def advance(self):
        groups, then = self.steps[self.now]
        for _, _, copies, receiver in groups:
            on(receiver, [copy.wait_recv for copy in copies])
        if then is not None:
            then()
        self.now += 1
        if self.now < len(self.steps):
            self.start()

    def settle(self):
        for groups, _ in self.steps:
            for copies, sender, arrivals, _ in groups:
                on(sender, [arrivals[0].wait_send])


def on(core, calls):
    def go():
        for call in calls:
            call()

    if core is None:
        go()
    else:
        pl.when(lax.axis_index(AXES[2]) == core)(go)


def gradients(predict, labels):
    exponent = jnp.exp(predict - jnp.max(predict, axis=0, keepdims=True))
    probability = exponent * (1.0 / jnp.sum(exponent, axis=0, keepdims=True))
    classes = lax.broadcasted_iota(jnp.int32, predict.shape, 0)
    gradient = jnp.where(classes == labels, probability - 1.0, probability)
    return gradient.astype(BF16), (probability * (1.0 - probability)).astype(BF16)


def leaf_slots(width):
    return [(lax.broadcasted_iota(jnp.int32, (16, width), 0) + 16 * j).astype(F32).astype(BF16) for j in range(4)]


def one_hot(ids, slots):
    shape = slots[0].shape
    one, zero = jnp.ones(shape, BF16), jnp.zeros(shape, BF16)
    ids = ids.astype(F32)
    rows = []
    for t in range(ids.shape[0]):
        held = jnp.broadcast_to(ids[t : t + 1], shape).astype(BF16)
        rows += [jnp.where(held == slot, one, zero) for slot in slots]
    return jnp.concatenate(rows, axis=0)


def half_sums(slot, ids, stacked, acc):
    rows = ids.shape[1] // 2
    slots = leaf_slots(TILE)
    trees = pl.ds(pl.multiple_of(slot // 2 * TREES_AT_ONCE, TREES_AT_ONCE), TREES_AT_ONCE)

    @pl.when(slot % 2 == 0)
    def _():
        acc[...] = jnp.zeros_like(acc)

    @pl.loop(0, rows, step=TILE * UNROLL)
    def _(first):
        total = None
        for u in range(UNROLL):
            cols = pl.ds(pl.multiple_of(slot % 2 * rows + first + u * TILE, TILE), TILE)
            matches = one_hot(ids[trees, cols], slots)
            part = lax.dot_general(
                matches, stacked[:, cols], (((1,), (1,)), ((), ())), preferred_element_type=F32
            )
            total = part if total is None else total + part
        acc[...] += total


def keep_sums(c, acc, sums):
    base = pl.multiple_of(c * WIDE, WIDE)
    sums[0, pl.ds(base, WIDE)] = acc[:, :LANES]
    sums[1, pl.ds(base, WIDE)] = acc[:, LANES:]


def class_major(values, first, table):
    for b in range(table.shape[1] // LANES):
        block = values[pl.ds(first + b * LANES, LANES)]
        table[:, b * LANES : (b + 1) * LANES] = block.T[: table.shape[0]].astype(BF16)


def plan():
    steps = lambda m: (1.5 + 0.4 * m, 9.0 + m, 8.5 + 0.5 * m, 1.5)
    ends = [sum(CHUNKS[: c + 1]) // TREES_AT_ONCE for c in range(len(CHUNKS))]
    newest = len(CHUNKS) - 1
    order, clock, due, now = [], 0.0, {}, {}
    waiting = []

    def advance(c):
        nonlocal clock
        clock = max(clock, due[c]) + 0.15
        now[c] += 1
        order.append(("advance", c))
        lengths = steps(CHUNKS[c] // TREES_AT_ONCE)
        if now[c] < len(lengths):
            due[c] = clock + lengths[now[c]]
        else:
            del due[c]
            waiting.append(c)

    for group in range(ends[-1]):
        for half in (0, 1):
            order.append(("sums", group, half))
            clock += HALF_US
            if half and group + 1 in ends:
                c = ends.index(group + 1)
                order.append(("start", c))
                now[c], due[c] = 0, clock + steps(CHUNKS[c] // TREES_AT_ONCE)[0]
            for c in sorted(due, key=due.get):
                if due[c] <= clock + EARLY_US:
                    advance(c)
    while newest in due:
        c = min(due, key=lambda c: due[c] - (0.3 if c == newest else 0.0))
        if waiting and due[c] - clock > APPLY_US * CHUNKS[waiting[0]] / 8 * 0.6:
            order.append(("apply", waiting.pop(0)))
            clock += APPLY_US * CHUNKS[order[-1][1]] / 8
        else:
            advance(c)
    order += [("advance", c) for c in due for _ in range(now[c], 4)]
    waiting += list(due)
    return order + [("apply", c) for c in waiting if c != newest]


def grow_kernel(predict, labels, ids, carried, values, *scratch):
    lbuf, ibuf, stacked, acc, table, sums, held = scratch[:7]
    bufs, send, recv, sems = scratch[7:-3], *scratch[-3:]
    classes, rows = predict.shape
    width = rows // PIECES

    def read(i):
        cols = pl.ds(pl.multiple_of(i * width, width), width)
        return pltpu.make_async_copy(predict.at[:, cols], carried.at[:, cols], sems.at[i])

    labels_read = pltpu.make_async_copy(labels, lbuf, sems.at[PIECES])
    ids_read = pltpu.make_async_copy(ids, ibuf, sems.at[PIECES + 1])
    labels_read.start()
    for i in range(PIECES):
        read(i).start()
    ids_read.start()
    greet()
    for k in (0, 1):
        stacked[k * LANES + 96 : (k + 1) * LANES] = jnp.zeros((LANES - 96, rows), BF16)
    labels_read.wait()

    @pl.loop(0, PIECES)
    def _(i):
        read(i).wait()

        @pl.loop(0, width, step=SOFTMAX)
        def _(first):
            cols = pl.ds(pl.multiple_of(i * width + first, SOFTMAX), SOFTMAX)
            gradient, hessian = gradients(carried[:, cols], lbuf[:, cols])
            stacked[:classes, cols] = gradient
            stacked[LANES : LANES + classes, cols] = hessian

    ids_read.wait()
    bases = [sum(CHUNKS[:c]) * LEAVES for c in range(len(CHUNKS))]
    chunks = [Exchange(c, CHUNKS[c], bases[c], sums, held, bufs, send, recv) for c in range(len(CHUNKS))]

    def apply(c):
        chunk = pl.ds(pl.multiple_of(c * WIDE, WIDE), WIDE)
        values[chunk] = held[chunk]
        class_major(held, pl.multiple_of(c * WIDE, WIDE), table)
        slots = leaf_slots(TILE)
        trees = pl.ds(pl.multiple_of(c * TREES_AT_ONCE, TREES_AT_ONCE), TREES_AT_ONCE)

        @pl.loop(0, rows, step=APPLY * TILE)
        def _(first):
            for u in range(APPLY):
                cols = pl.ds(pl.multiple_of(first + u * TILE, TILE), TILE)
                update = jnp.dot(table[...], one_hot(ibuf[trees, cols], slots), preferred_element_type=F32)
                carried[:, cols] += update[:classes]

    def exchange(actions):
        for what, c in actions:
            getattr(chunks[c], what)()

    parts = [[]]
    for action in plan():
        if action[0] in ("sums", "apply"):
            parts.append([])
        else:
            parts[-1].append(action)
    halves = 2 * len(chunks)

    @pl.loop(0, halves)
    def _(slot):
        half_sums(slot, ibuf, stacked, acc)

        @pl.when(slot % 2 == 1)
        def _():
            keep_sums(slot // 2, acc, sums)

        for k in range(halves - 1):
            if parts[k + 1]:

                @pl.when(slot == k)
                def _():
                    if k == 1:
                        wait_for_all()
                    exchange(parts[k + 1])

    exchange(parts[halves])

    @pl.loop(0, len(chunks) - 1)
    def _(c):
        apply(c)
        for k in range(len(chunks) - 1):
            if parts[halves + 1 + k]:

                @pl.when(c == k)
                def _():
                    exchange(parts[halves + 1 + k])

    values[-WIDE:] = held[-WIDE:]
    for chunk in chunks:
        chunk.settle()


def grow(predict, labels, ids):
    classes, rows = predict.shape
    leaves = ids.shape[0] * LEAVES
    k = len(CHUNKS)
    pinned = [pltpu.with_memory_space_constraint(a, pltpu.HBM) for a in (predict, labels, ids)]
    return pl.pallas_call(
        grow_kernel,
        out_shape=(jax.ShapeDtypeStruct(predict.shape, F32), jax.ShapeDtypeStruct((leaves, LANES), F32)),
        in_specs=[pl.BlockSpec(memory_space=pltpu.HBM)] * 3,
        out_specs=(pl.BlockSpec(memory_space=pltpu.VMEM), pl.BlockSpec(memory_space=pltpu.VMEM)),
        scratch_shapes=[
            pltpu.VMEM((1, rows), jnp.int32),
            pltpu.VMEM(ids.shape, jnp.int32),
            pltpu.VMEM((2 * LANES, rows), BF16),
            pltpu.VMEM((WIDE, 2 * LANES), F32),
            pltpu.VMEM((112, WIDE), BF16),
            pltpu.VMEM((2, leaves, LANES), F32),
            pltpu.VMEM((leaves, LANES), F32),
            pltpu.VMEM((leaves, LANES), F32),
            pltpu.VMEM((leaves, LANES), F32),
            pltpu.VMEM((k, 2, 64, leaves // k // 64, LANES), F32),
            pltpu.SemaphoreType.DMA((k, COPIES)),
            pltpu.SemaphoreType.DMA((k, COPIES)),
            pltpu.SemaphoreType.DMA((PIECES + 2,)),
        ],
        compiler_params=pltpu.CompilerParams(
            collective_id=0, has_side_effects=True, vmem_limit_bytes=40 << 20
        ),
        name="grow",
    )(*pinned)


def finish_kernel(values, carried, ids, out, own, table, ibuf, obuf, sems, ids_sem):
    classes, rows = carried.shape
    width = rows // WRITES
    first_id = ids.shape[0] - CHUNKS[-1]
    ids_read = pltpu.make_async_copy(ids.at[pl.ds(first_id, CHUNKS[-1])], ibuf, ids_sem)
    ids_read.start()
    class_major(values, first_id * LEAVES, table)
    ids_read.wait()
    slots = leaf_slots(TILE)
    writes = []
    for i in range(WRITES):
        for u in range(width // TILE):
            cols = pl.ds(i * width + u * TILE, TILE)
            update = jnp.dot(table[...], one_hot(ibuf[:, cols], slots), preferred_element_type=F32)
            obuf[:, cols] = carried[:, cols] + update[:classes]
        cols = pl.ds(i * width, width)
        writes.append(pltpu.make_async_copy(obuf.at[:, cols], out.at[:, cols], sems.at[i]))
        writes[-1].start()
    own_width = own.shape[1]
    for b in range(own_width // LANES):
        first = pl.multiple_of(lax.axis_index("leaf") * own_width + b * LANES, LANES)
        own[:, b * LANES : (b + 1) * LANES] = values[pl.ds(first, LANES)].T[:classes]
    for write in writes:
        write.wait()


def finish(values, carried, ids):
    classes, rows = carried.shape
    own_width = values.shape[0] // lax.axis_size("leaf")
    return pl.pallas_call(
        finish_kernel,
        out_shape=(
            jax.ShapeDtypeStruct(carried.shape, F32),
            jax.ShapeDtypeStruct((classes, own_width), F32),
        ),
        in_specs=[
            pl.BlockSpec(memory_space=pltpu.VMEM),
            pl.BlockSpec(memory_space=pltpu.VMEM),
            pl.BlockSpec(memory_space=pl.ANY),
        ],
        out_specs=(pl.BlockSpec(memory_space=pl.ANY), pl.BlockSpec(memory_space=pltpu.VMEM)),
        scratch_shapes=[
            pltpu.VMEM((112, CHUNKS[-1] * LEAVES), BF16),
            pltpu.VMEM((CHUNKS[-1], rows), jnp.int32),
            pltpu.VMEM((classes, rows), F32),
            pltpu.SemaphoreType.DMA((WRITES,)),
            pltpu.SemaphoreType.DMA,
        ],
        compiler_params=pltpu.CompilerParams(vmem_limit_bytes=24 << 20),
        name="finish",
    )(values, carried, ids)


def shards(predict, labels, leaf_ids):
    carried, values = grow(predict, labels[None, :], leaf_ids)
    return finish(values, carried, leaf_ids)


def solution(mesh):
    finer = Mesh(mesh.devices.reshape(4, 4, 2, mesh.shape["leaf"]), AXES)
    in_specs = (P(None, AXES), P(AXES), P(None, AXES))
    out_specs = (P(None, AXES), P(None, "leaf"))
    return jax.shard_map(shards, mesh=finer, in_specs=in_specs, out_specs=out_specs, check_vma=False)
```

```python
import jax
import jax.numpy as jnp
from jax import lax
from jax.experimental import pallas as pl
from jax.experimental.pallas import tpu as pltpu
from jax.sharding import Mesh
from jax.sharding import PartitionSpec as P

F32, BF16 = jnp.float32, jnp.bfloat16
LEAVES = 64
AXES = ("dp_0", "dp_1", "dp_2", "leaf")
TREES_AT_ONCE = 8
WIDE = TREES_AT_ONCE * LEAVES
LANES = 128
CHUNKS = (8, 8, 8, 8)
COPIES = 6
TILE = 256
PIECES = 8
APPLY = 32
WRITES = 4
UNROLL = 16
SOFTMAX = 1024
HALF_US, APPLY_US, EARLY_US = 1.15, 1.9, 0.8

step_size = 0.5
ridge_term = 1.0


def places():
    y, x, core, z = (lax.axis_index(name) for name in AXES)
    return x, y, z, core


def partner():
    x, y, z, core = places()
    return (y, x, 1 - core, z)


def moves():
    found = [(a, b, c) for a in range(4) for b in range(4) for c in range(4)][1:]
    return sorted(found, key=lambda move: -sum(min(m, 4 - m) for m in move))


def chip_at(move, core):
    x, y, z, _ = places()
    a, b, c = ((at + m) % 4 for at, m in zip((x, y, z), move))
    return (b, a, core, c), a * 16 + b * 4 + c


def greet():
    barrier = pltpu.get_barrier_semaphore()

    def call(core):
        peers = [partner()] if core == 1 else []
        for peer in peers + [chip_at(move, core)[0] for move in moves()]:
            pl.semaphore_signal(barrier, inc=1, device_id=peer, device_id_type=pl.DeviceIdType.MESH)

    call(1)

    @pl.when(lax.axis_index(AXES[2]) == 1)
    def _():
        call(0)


def wait_for_all():
    pl.semaphore_wait(pltpu.get_barrier_semaphore(), 64 + 63 * lax.axis_index(AXES[2]))


class Exchange:
    def __init__(self, c, trees, base, sums, held, bufs, send, recv):
        paired, summed, last = bufs
        x, y, z, core = places()
        size = trees * LEAVES
        rows = size // 64
        whole = pl.ds(base, size)

        def copy(i, src, dst, peer, lands=None):
            return pltpu.make_async_remote_copy(
                src_ref=src,
                dst_ref=dst,
                send_sem=send.at[c, i],
                recv_sem=recv.at[c, i if lands is None else lands],
                device_id=peer,
                device_id_type=pl.DeviceIdType.MESH,
            )

        def block(chip):
            return pl.ds(pl.multiple_of(base + chip * rows, 8), rows)

        own = block(x * 16 + y * 4 + z)
        pieces, rounds = [], []
        for n, move in enumerate(moves()):
            peer, chip = chip_at(move, 1)
            pieces.append(copy(1, summed.at[block(chip)], last.at[c, core, n], peer, 2 - core))
            rounds.append(copy(4, held.at[own], held.at[own], peer))
        others = pl.ds(0, 63)
        arrived = [copy(1, last.at[c, k, others], last.at[c, k, others], partner(), 2 - k) for k in (0, 1)]
        beside = copy(3, summed.at[own], last.at[c, 0, 63], partner())
        rest = held.at[pl.ds(base, size - rows)]
        first = copy(0, sums.at[1 - core, whole], paired.at[whole], partner())
        forward = copy(5, held.at[whole], held.at[whole], partner())

        def add_pair():
            summed[whole] = sums[core, whole] + paired[whole]

        def solve():
            @pl.when(core == 1)
            def _():
                last[c, 1, 63] = summed[own]
                grad, hess = (jnp.sum(last[c, k], axis=0) for k in (0, 1))
                held[own] = -step_size * grad / (hess + ridge_term)

        self.steps = [
            ([([first], None, [first], None)], add_pair),
            ([(pieces, None, arrived, 1), ([beside], 0, [beside], 1)], solve),
            ([(rounds, 1, [copy(4, rest, rest, partner())], 1)], None),
            ([([forward], 1, [forward], 0)], None),
        ]
        self.now = 0

    def start(self):
        for copies, sender, _, _ in self.steps[self.now][0]:
            on(sender, [copy.start for copy in copies])

    def advance(self):
        groups, then = self.steps[self.now]
        for _, _, copies, receiver in groups:
            on(receiver, [copy.wait_recv for copy in copies])
        if then is not None:
            then()
        self.now += 1
        if self.now < len(self.steps):
            self.start()

    def settle(self):
        for groups, _ in self.steps:
            for copies, sender, arrivals, _ in groups:
                on(sender, [arrivals[0].wait_send])


def on(core, calls):
    def go():
        for call in calls:
            call()

    if core is None:
        go()
    else:
        pl.when(lax.axis_index(AXES[2]) == core)(go)


def gradients(predict, labels):
    exponent = jnp.exp(predict - jnp.max(predict, axis=0, keepdims=True))
    probability = exponent * (1.0 / jnp.sum(exponent, axis=0, keepdims=True))
    classes = lax.broadcasted_iota(jnp.int32, predict.shape, 0)
    gradient = jnp.where(classes == labels, probability - 1.0, probability)
    return gradient.astype(BF16), (probability * (1.0 - probability)).astype(BF16)


def leaf_slots(width):
    return [(lax.broadcasted_iota(jnp.int32, (16, width), 0) + 16 * j).astype(F32).astype(BF16) for j in range(4)]


def one_hot(ids, slots):
    shape = slots[0].shape
    one, zero = jnp.ones(shape, BF16), jnp.zeros(shape, BF16)
    ids = ids.astype(F32)
    rows = []
    for t in range(ids.shape[0]):
        held = jnp.broadcast_to(ids[t : t + 1], shape).astype(BF16)
        rows += [jnp.where(held == slot, one, zero) for slot in slots]
    return jnp.concatenate(rows, axis=0)


def half_sums(slot, ids, stacked, acc):
    rows = ids.shape[1] // 2
    slots = leaf_slots(TILE)
    trees = pl.ds(pl.multiple_of(slot // 2 * TREES_AT_ONCE, TREES_AT_ONCE), TREES_AT_ONCE)

    @pl.when(slot % 2 == 0)
    def _():
        acc[...] = jnp.zeros_like(acc)

    @pl.loop(0, rows, step=TILE * UNROLL)
    def _(first):
        total = None
        for u in range(UNROLL):
            cols = pl.ds(pl.multiple_of(slot % 2 * rows + first + u * TILE, TILE), TILE)
            matches = one_hot(ids[trees, cols], slots)
            part = lax.dot_general(
                matches, stacked[:, cols], (((1,), (1,)), ((), ())), preferred_element_type=F32
            )
            total = part if total is None else total + part
        acc[...] += total


def keep_sums(c, acc, sums):
    base = pl.multiple_of(c * WIDE, WIDE)
    sums[0, pl.ds(base, WIDE)] = acc[:, :LANES]
    sums[1, pl.ds(base, WIDE)] = acc[:, LANES:]


def class_major(values, first, table):
    for b in range(table.shape[1] // LANES):
        block = values[pl.ds(first + b * LANES, LANES)]
        table[:, b * LANES : (b + 1) * LANES] = block.T[: table.shape[0]].astype(BF16)


def plan():
    steps = lambda m: (1.5 + 0.4 * m, 9.0 + m, 8.5 + 0.5 * m, 1.5)
    ends = [sum(CHUNKS[: c + 1]) // TREES_AT_ONCE for c in range(len(CHUNKS))]
    newest = len(CHUNKS) - 1
    order, clock, due, now = [], 0.0, {}, {}
    waiting = []

    def advance(c):
        nonlocal clock
        clock = max(clock, due[c]) + 0.15
        now[c] += 1
        order.append(("advance", c))
        lengths = steps(CHUNKS[c] // TREES_AT_ONCE)
        if now[c] < len(lengths):
            due[c] = clock + lengths[now[c]]
        else:
            del due[c]
            waiting.append(c)

    for group in range(ends[-1]):
        for half in (0, 1):
            order.append(("sums", group, half))
            clock += HALF_US
            if half and group + 1 in ends:
                c = ends.index(group + 1)
                order.append(("start", c))
                now[c], due[c] = 0, clock + steps(CHUNKS[c] // TREES_AT_ONCE)[0]
            for c in sorted(due, key=due.get):
                if due[c] <= clock + EARLY_US:
                    advance(c)
    while newest in due:
        c = min(due, key=lambda c: due[c] - (0.3 if c == newest else 0.0))
        if waiting and due[c] - clock > APPLY_US * CHUNKS[waiting[0]] / 8 * 0.6:
            order.append(("apply", waiting.pop(0)))
            clock += APPLY_US * CHUNKS[order[-1][1]] / 8
        else:
            advance(c)
    order += [("advance", c) for c in due for _ in range(now[c], 4)]
    waiting += list(due)
    return order + [("apply", c) for c in waiting if c != newest]


def grow_kernel(predict, labels, ids, carried, values, *scratch):
    lbuf, ibuf, stacked, acc, table, sums, held = scratch[:7]
    bufs, send, recv, sems = scratch[7:-3], *scratch[-3:]
    classes, rows = predict.shape
    width = rows // PIECES

    def read(i):
        cols = pl.ds(pl.multiple_of(i * width, width), width)
        return pltpu.make_async_copy(predict.at[:, cols], carried.at[:, cols], sems.at[i])

    labels_read = pltpu.make_async_copy(labels, lbuf, sems.at[PIECES])
    ids_read = pltpu.make_async_copy(ids, ibuf, sems.at[PIECES + 1])
    labels_read.start()
    for i in range(PIECES):
        read(i).start()
    ids_read.start()
    greet()
    for k in (0, 1):
        stacked[k * LANES + 96 : (k + 1) * LANES] = jnp.zeros((LANES - 96, rows), BF16)
    labels_read.wait()

    @pl.loop(0, PIECES)
    def _(i):
        read(i).wait()

        @pl.loop(0, width, step=SOFTMAX)
        def _(first):
            cols = pl.ds(pl.multiple_of(i * width + first, SOFTMAX), SOFTMAX)
            gradient, hessian = gradients(carried[:, cols], lbuf[:, cols])
            stacked[:classes, cols] = gradient
            stacked[LANES : LANES + classes, cols] = hessian

    ids_read.wait()
    bases = [sum(CHUNKS[:c]) * LEAVES for c in range(len(CHUNKS))]
    chunks = [Exchange(c, CHUNKS[c], bases[c], sums, held, bufs, send, recv) for c in range(len(CHUNKS))]

    def apply(c):
        chunk = pl.ds(pl.multiple_of(c * WIDE, WIDE), WIDE)
        values[chunk] = held[chunk]
        class_major(held, pl.multiple_of(c * WIDE, WIDE), table)
        slots = leaf_slots(TILE)
        trees = pl.ds(pl.multiple_of(c * TREES_AT_ONCE, TREES_AT_ONCE), TREES_AT_ONCE)

        @pl.loop(0, rows, step=APPLY * TILE)
        def _(first):
            for u in range(APPLY):
                cols = pl.ds(pl.multiple_of(first + u * TILE, TILE), TILE)
                update = jnp.dot(table[...], one_hot(ibuf[trees, cols], slots), preferred_element_type=F32)
                carried[:, cols] += update[:classes]

    def exchange(actions):
        for what, c in actions:
            getattr(chunks[c], what)()

    parts = [[]]
    for action in plan():
        if action[0] in ("sums", "apply"):
            parts.append([])
        else:
            parts[-1].append(action)
    halves = 2 * len(chunks)

    @pl.loop(0, halves)
    def _(slot):
        half_sums(slot, ibuf, stacked, acc)

        @pl.when(slot % 2 == 1)
        def _():
            keep_sums(slot // 2, acc, sums)

        for k in range(halves - 1):
            if parts[k + 1]:

                @pl.when(slot == k)
                def _():
                    if k == 1:
                        wait_for_all()
                    exchange(parts[k + 1])

    exchange(parts[halves])

    @pl.loop(0, len(chunks) - 1)
    def _(c):
        apply(c)
        for k in range(len(chunks) - 1):
            if parts[halves + 1 + k]:

                @pl.when(c == k)
                def _():
                    exchange(parts[halves + 1 + k])

    values[-WIDE:] = held[-WIDE:]
    for chunk in chunks:
        chunk.settle()


def grow(predict, labels, ids):
    classes, rows = predict.shape
    leaves = ids.shape[0] * LEAVES
    k = len(CHUNKS)
    pinned = [pltpu.with_memory_space_constraint(a, pltpu.HBM) for a in (predict, labels, ids)]
    return pl.pallas_call(
        grow_kernel,
        out_shape=(jax.ShapeDtypeStruct(predict.shape, F32), jax.ShapeDtypeStruct((leaves, LANES), F32)),
        in_specs=[pl.BlockSpec(memory_space=pltpu.HBM)] * 3,
        out_specs=(pl.BlockSpec(memory_space=pltpu.VMEM), pl.BlockSpec(memory_space=pltpu.VMEM)),
        scratch_shapes=[
            pltpu.VMEM((1, rows), jnp.int32),
            pltpu.VMEM(ids.shape, jnp.int32),
            pltpu.VMEM((2 * LANES, rows), BF16),
            pltpu.VMEM((WIDE, 2 * LANES), F32),
            pltpu.VMEM((112, WIDE), BF16),
            pltpu.VMEM((2, leaves, LANES), F32),
            pltpu.VMEM((leaves, LANES), F32),
            pltpu.VMEM((leaves, LANES), F32),
            pltpu.VMEM((leaves, LANES), F32),
            pltpu.VMEM((k, 2, 64, leaves // k // 64, LANES), F32),
            pltpu.SemaphoreType.DMA((k, COPIES)),
            pltpu.SemaphoreType.DMA((k, COPIES)),
            pltpu.SemaphoreType.DMA((PIECES + 2,)),
        ],
        compiler_params=pltpu.CompilerParams(
            collective_id=0, has_side_effects=True, vmem_limit_bytes=40 << 20
        ),
        name="grow",
    )(*pinned)


def finish_kernel(values, carried, ids, out, own, table, ibuf, obuf, sems, ids_sem):
    classes, rows = carried.shape
    width = rows // WRITES
    first_id = ids.shape[0] - CHUNKS[-1]
    ids_read = pltpu.make_async_copy(ids.at[pl.ds(first_id, CHUNKS[-1])], ibuf, ids_sem)
    ids_read.start()
    class_major(values, first_id * LEAVES, table)
    ids_read.wait()
    slots = leaf_slots(TILE)
    writes = []
    for i in range(WRITES):
        for u in range(width // TILE):
            cols = pl.ds(i * width + u * TILE, TILE)
            update = jnp.dot(table[...], one_hot(ibuf[:, cols], slots), preferred_element_type=F32)
            obuf[:, cols] = carried[:, cols] + update[:classes]
        cols = pl.ds(i * width, width)
        writes.append(pltpu.make_async_copy(obuf.at[:, cols], out.at[:, cols], sems.at[i]))
        writes[-1].start()
    own_width = own.shape[1]
    for b in range(own_width // LANES):
        first = pl.multiple_of(lax.axis_index("leaf") * own_width + b * LANES, LANES)
        own[:, b * LANES : (b + 1) * LANES] = values[pl.ds(first, LANES)].T[:classes]
    for write in writes:
        write.wait()


def finish(values, carried, ids):
    classes, rows = carried.shape
    own_width = values.shape[0] // lax.axis_size("leaf")
    return pl.pallas_call(
        finish_kernel,
        out_shape=(
            jax.ShapeDtypeStruct(carried.shape, F32),
            jax.ShapeDtypeStruct((classes, own_width), F32),
        ),
        in_specs=[
            pl.BlockSpec(memory_space=pltpu.VMEM),
            pl.BlockSpec(memory_space=pltpu.VMEM),
            pl.BlockSpec(memory_space=pl.ANY),
        ],
        out_specs=(pl.BlockSpec(memory_space=pl.ANY), pl.BlockSpec(memory_space=pltpu.VMEM)),
        scratch_shapes=[
            pltpu.VMEM((112, CHUNKS[-1] * LEAVES), BF16),
            pltpu.VMEM((CHUNKS[-1], rows), jnp.int32),
            pltpu.VMEM((classes, rows), F32),
            pltpu.SemaphoreType.DMA((WRITES,)),
            pltpu.SemaphoreType.DMA,
        ],
        compiler_params=pltpu.CompilerParams(vmem_limit_bytes=24 << 20),
        name="finish",
    )(values, carried, ids)


def shards(predict, labels, leaf_ids):
    carried, values = grow(predict, labels[None, :], leaf_ids)
    return finish(values, carried, leaf_ids)


def solution(mesh):
    finer = Mesh(mesh.devices.reshape(4, 4, 2, mesh.shape["leaf"]), AXES)
    in_specs = (P(None, AXES), P(AXES), P(None, AXES))
    out_specs = (P(None, AXES), P(None, "leaf"))
    return jax.shard_map(shards, mesh=finer, in_specs=in_specs, out_specs=out_specs, check_vma=False)
```

```python
import jax
import jax.numpy as jnp
from jax import lax
from jax.experimental import pallas as pl
from jax.experimental.pallas import tpu as pltpu
from jax.sharding import Mesh
from jax.sharding import PartitionSpec as P

F32, BF16 = jnp.float32, jnp.bfloat16
LEAVES = 64
AXES = ("dp_0", "dp_1", "dp_2", "leaf")
TREES_AT_ONCE = 8
WIDE = TREES_AT_ONCE * LEAVES
LANES = 128
CHUNKS = (8, 8, 8, 8)
COPIES = 6
TILE = 256
PIECES = 8
APPLY = 32
WRITES = 4
UNROLL = 16
SOFTMAX = 1024
HALF_US, APPLY_US, EARLY_US = 1.15, 1.9, 0.8

step_size = 0.5
ridge_term = 1.0


def places():
    y, x, core, z = (lax.axis_index(name) for name in AXES)
    return x, y, z, core


def partner():
    x, y, z, core = places()
    return (y, x, 1 - core, z)


def moves():
    found = [(a, b, c) for a in range(4) for b in range(4) for c in range(4)][1:]
    return sorted(found, key=lambda move: -sum(min(m, 4 - m) for m in move))


def chip_at(move, core):
    x, y, z, _ = places()
    a, b, c = ((at + m) % 4 for at, m in zip((x, y, z), move))
    return (b, a, core, c), a * 16 + b * 4 + c


def greet():
    barrier = pltpu.get_barrier_semaphore()

    def call(core):
        peers = [partner()] if core == 1 else []
        for peer in peers + [chip_at(move, core)[0] for move in moves()]:
            pl.semaphore_signal(barrier, inc=1, device_id=peer, device_id_type=pl.DeviceIdType.MESH)

    call(1)

    @pl.when(lax.axis_index(AXES[2]) == 1)
    def _():
        call(0)


def wait_for_all():
    pl.semaphore_wait(pltpu.get_barrier_semaphore(), 64 + 63 * lax.axis_index(AXES[2]))


class Exchange:
    def __init__(self, c, trees, base, sums, held, bufs, send, recv):
        paired, summed, last = bufs
        x, y, z, core = places()
        size = trees * LEAVES
        rows = size // 64
        whole = pl.ds(base, size)

        def copy(i, src, dst, peer, lands=None):
            return pltpu.make_async_remote_copy(
                src_ref=src,
                dst_ref=dst,
                send_sem=send.at[c, i],
                recv_sem=recv.at[c, i if lands is None else lands],
                device_id=peer,
                device_id_type=pl.DeviceIdType.MESH,
            )

        def block(chip):
            return pl.ds(pl.multiple_of(base + chip * rows, 8), rows)

        own = block(x * 16 + y * 4 + z)
        pieces, rounds = [], []
        for n, move in enumerate(moves()):
            peer, chip = chip_at(move, 1)
            pieces.append(copy(1, summed.at[block(chip)], last.at[c, core, n], peer, 2 - core))
            rounds.append(copy(4, held.at[own], held.at[own], peer))
        others = pl.ds(0, 63)
        arrived = [copy(1, last.at[c, k, others], last.at[c, k, others], partner(), 2 - k) for k in (0, 1)]
        beside = copy(3, summed.at[own], last.at[c, 0, 63], partner())
        rest = held.at[pl.ds(base, size - rows)]
        first = copy(0, sums.at[1 - core, whole], paired.at[whole], partner())
        forward = copy(5, held.at[whole], held.at[whole], partner())

        def add_pair():
            summed[whole] = sums[core, whole] + paired[whole]

        def solve():
            @pl.when(core == 1)
            def _():
                last[c, 1, 63] = summed[own]
                grad, hess = (jnp.sum(last[c, k], axis=0) for k in (0, 1))
                held[own] = -step_size * grad / (hess + ridge_term)

        self.steps = [
            ([([first], None, [first], None)], add_pair),
            ([(pieces, None, arrived, 1), ([beside], 0, [beside], 1)], solve),
            ([(rounds, 1, [copy(4, rest, rest, partner())], 1)], None),
            ([([forward], 1, [forward], 0)], None),
        ]
        self.now = 0

    def start(self):
        for copies, sender, _, _ in self.steps[self.now][0]:
            on(sender, [copy.start for copy in copies])

    def advance(self):
        groups, then = self.steps[self.now]
        for _, _, copies, receiver in groups:
            on(receiver, [copy.wait_recv for copy in copies])
        if then is not None:
            then()
        self.now += 1
        if self.now < len(self.steps):
            self.start()

    def settle(self):
        for groups, _ in self.steps:
            for copies, sender, arrivals, _ in groups:
                on(sender, [arrivals[0].wait_send])


def on(core, calls):
    def go():
        for call in calls:
            call()

    if core is None:
        go()
    else:
        pl.when(lax.axis_index(AXES[2]) == core)(go)


def gradients(predict, labels):
    exponent = jnp.exp(predict - jnp.max(predict, axis=0, keepdims=True))
    probability = exponent * (1.0 / jnp.sum(exponent, axis=0, keepdims=True))
    classes = lax.broadcasted_iota(jnp.int32, predict.shape, 0)
    gradient = jnp.where(classes == labels, probability - 1.0, probability)
    return gradient.astype(BF16), (probability * (1.0 - probability)).astype(BF16)


def leaf_slots(width):
    return [(lax.broadcasted_iota(jnp.int32, (16, width), 0) + 16 * j).astype(F32).astype(BF16) for j in range(4)]


def one_hot(ids, slots):
    shape = slots[0].shape
    one, zero = jnp.ones(shape, BF16), jnp.zeros(shape, BF16)
    ids = ids.astype(F32)
    rows = []
    for t in range(ids.shape[0]):
        held = jnp.broadcast_to(ids[t : t + 1], shape).astype(BF16)
        rows += [jnp.where(held == slot, one, zero) for slot in slots]
    return jnp.concatenate(rows, axis=0)


def half_sums(slot, ids, stacked, acc):
    rows = ids.shape[1] // 2
    slots = leaf_slots(TILE)
    trees = pl.ds(pl.multiple_of(slot // 2 * TREES_AT_ONCE, TREES_AT_ONCE), TREES_AT_ONCE)

    @pl.loop(0, rows, step=TILE * UNROLL)
    def _(first):
        total = None
        for u in range(UNROLL):
            cols = pl.ds(pl.multiple_of(slot % 2 * rows + first + u * TILE, TILE), TILE)
            matches = one_hot(ids[trees, cols], slots)
            part = lax.dot_general(
                matches, stacked[:, cols], (((1,), (1,)), ((), ())), preferred_element_type=F32
            )
            total = part if total is None else total + part
        fresh = jnp.logical_and(slot % 2 == 0, first == 0)

        @pl.when(fresh)
        def _():
            acc[...] = total

        @pl.when(jnp.logical_not(fresh))
        def _():
            acc[...] += total


def keep_sums(c, acc, sums):
    base = pl.multiple_of(c * WIDE, WIDE)
    sums[0, pl.ds(base, WIDE)] = acc[:, :LANES]
    sums[1, pl.ds(base, WIDE)] = acc[:, LANES:]


def class_major(values, first, table):
    for b in range(table.shape[1] // LANES):
        block = values[pl.ds(first + b * LANES, LANES)]
        table[:, b * LANES : (b + 1) * LANES] = block.T[: table.shape[0]].astype(BF16)


def plan():
    steps = lambda m: (1.5 + 0.4 * m, 9.0 + m, 8.5 + 0.5 * m, 1.5)
    ends = [sum(CHUNKS[: c + 1]) // TREES_AT_ONCE for c in range(len(CHUNKS))]
    newest = len(CHUNKS) - 1
    order, clock, due, now = [], 0.0, {}, {}
    waiting = []

    def advance(c):
        nonlocal clock
        clock = max(clock, due[c]) + 0.15
        now[c] += 1
        order.append(("advance", c))
        lengths = steps(CHUNKS[c] // TREES_AT_ONCE)
        if now[c] < len(lengths):
            due[c] = clock + lengths[now[c]]
        else:
            del due[c]
            waiting.append(c)

    for group in range(ends[-1]):
        for half in (0, 1):
            order.append(("sums", group, half))
            clock += HALF_US
            if half and group + 1 in ends:
                c = ends.index(group + 1)
                order.append(("start", c))
                now[c], due[c] = 0, clock + steps(CHUNKS[c] // TREES_AT_ONCE)[0]
            for c in sorted(due, key=due.get):
                if due[c] <= clock + EARLY_US:
                    advance(c)
    while newest in due:
        c = min(due, key=lambda c: due[c] - (0.3 if c == newest else 0.0))
        if waiting and due[c] - clock > APPLY_US * CHUNKS[waiting[0]] / 8 * 0.6:
            order.append(("apply", waiting.pop(0)))
            clock += APPLY_US * CHUNKS[order[-1][1]] / 8
        else:
            advance(c)
    order += [("advance", c) for c in due for _ in range(now[c], 4)]
    waiting += list(due)
    return order + [("apply", c) for c in waiting if c != newest]


def grow_kernel(predict, labels, ids, carried, values, *scratch):
    lbuf, ibuf, stacked, acc, table, sums, held = scratch[:7]
    bufs, send, recv, sems = scratch[7:-3], *scratch[-3:]
    classes, rows = predict.shape
    width = rows // PIECES

    def read(i):
        cols = pl.ds(pl.multiple_of(i * width, width), width)
        return pltpu.make_async_copy(predict.at[:, cols], carried.at[:, cols], sems.at[i])

    labels_read = pltpu.make_async_copy(labels, lbuf, sems.at[PIECES])
    ids_read = pltpu.make_async_copy(ids, ibuf, sems.at[PIECES + 1])
    labels_read.start()
    for i in range(PIECES):
        read(i).start()
    ids_read.start()
    greet()
    for k in (0, 1):
        stacked[k * LANES + 96 : (k + 1) * LANES] = jnp.zeros((LANES - 96, rows), BF16)
    labels_read.wait()

    @pl.loop(0, PIECES)
    def _(i):
        read(i).wait()

        @pl.loop(0, width, step=SOFTMAX)
        def _(first):
            cols = pl.ds(pl.multiple_of(i * width + first, SOFTMAX), SOFTMAX)
            gradient, hessian = gradients(carried[:, cols], lbuf[:, cols])
            stacked[:classes, cols] = gradient
            stacked[LANES : LANES + classes, cols] = hessian

    ids_read.wait()
    bases = [sum(CHUNKS[:c]) * LEAVES for c in range(len(CHUNKS))]
    chunks = [Exchange(c, CHUNKS[c], bases[c], sums, held, bufs, send, recv) for c in range(len(CHUNKS))]

    def apply(c):
        chunk = pl.ds(pl.multiple_of(c * WIDE, WIDE), WIDE)
        values[chunk] = held[chunk]
        class_major(held, pl.multiple_of(c * WIDE, WIDE), table)
        slots = leaf_slots(TILE)
        trees = pl.ds(pl.multiple_of(c * TREES_AT_ONCE, TREES_AT_ONCE), TREES_AT_ONCE)

        @pl.loop(0, rows, step=APPLY * TILE)
        def _(first):
            for u in range(APPLY):
                cols = pl.ds(pl.multiple_of(first + u * TILE, TILE), TILE)
                update = jnp.dot(table[...], one_hot(ibuf[trees, cols], slots), preferred_element_type=F32)
                carried[:, cols] += update[:classes]

    def exchange(actions):
        for what, c in actions:
            getattr(chunks[c], what)()

    parts = [[]]
    for action in plan():
        if action[0] in ("sums", "apply"):
            parts.append([])
        else:
            parts[-1].append(action)
    halves = 2 * len(chunks)

    @pl.loop(0, halves)
    def _(slot):
        half_sums(slot, ibuf, stacked, acc)

        @pl.when(slot % 2 == 1)
        def _():
            keep_sums(slot // 2, acc, sums)

        for k in range(halves - 1):
            if parts[k + 1]:

                @pl.when(slot == k)
                def _():
                    if k == 1:
                        wait_for_all()
                    exchange(parts[k + 1])

    exchange(parts[halves])

    @pl.loop(0, len(chunks) - 1)
    def _(c):
        apply(c)
        for k in range(len(chunks) - 1):
            if parts[halves + 1 + k]:

                @pl.when(c == k)
                def _():
                    exchange(parts[halves + 1 + k])

    values[-WIDE:] = held[-WIDE:]
    for chunk in chunks:
        chunk.settle()


def grow(predict, labels, ids):
    classes, rows = predict.shape
    leaves = ids.shape[0] * LEAVES
    k = len(CHUNKS)
    pinned = [pltpu.with_memory_space_constraint(a, pltpu.HBM) for a in (predict, labels, ids)]
    return pl.pallas_call(
        grow_kernel,
        out_shape=(jax.ShapeDtypeStruct(predict.shape, F32), jax.ShapeDtypeStruct((leaves, LANES), F32)),
        in_specs=[pl.BlockSpec(memory_space=pltpu.HBM)] * 3,
        out_specs=(pl.BlockSpec(memory_space=pltpu.VMEM), pl.BlockSpec(memory_space=pltpu.VMEM)),
        scratch_shapes=[
            pltpu.VMEM((1, rows), jnp.int32),
            pltpu.VMEM(ids.shape, jnp.int32),
            pltpu.VMEM((2 * LANES, rows), BF16),
            pltpu.VMEM((WIDE, 2 * LANES), F32),
            pltpu.VMEM((112, WIDE), BF16),
            pltpu.VMEM((2, leaves, LANES), F32),
            pltpu.VMEM((leaves, LANES), F32),
            pltpu.VMEM((leaves, LANES), F32),
            pltpu.VMEM((leaves, LANES), F32),
            pltpu.VMEM((k, 2, 64, leaves // k // 64, LANES), F32),
            pltpu.SemaphoreType.DMA((k, COPIES)),
            pltpu.SemaphoreType.DMA((k, COPIES)),
            pltpu.SemaphoreType.DMA((PIECES + 2,)),
        ],
        compiler_params=pltpu.CompilerParams(
            collective_id=0, has_side_effects=True, vmem_limit_bytes=40 << 20
        ),
        name="grow",
    )(*pinned)


def finish_kernel(values, carried, ids, out, own, table, ibuf, obuf, sems, ids_sem):
    classes, rows = carried.shape
    width = rows // WRITES
    first_id = ids.shape[0] - CHUNKS[-1]
    ids_read = pltpu.make_async_copy(ids.at[pl.ds(first_id, CHUNKS[-1])], ibuf, ids_sem)
    ids_read.start()
    class_major(values, first_id * LEAVES, table)
    ids_read.wait()
    slots = leaf_slots(TILE)
    writes = []
    for i in range(WRITES):
        for u in range(width // TILE):
            cols = pl.ds(i * width + u * TILE, TILE)
            update = jnp.dot(table[...], one_hot(ibuf[:, cols], slots), preferred_element_type=F32)
            obuf[:, cols] = carried[:, cols] + update[:classes]
        cols = pl.ds(i * width, width)
        writes.append(pltpu.make_async_copy(obuf.at[:, cols], out.at[:, cols], sems.at[i]))
        writes[-1].start()
    own_width = own.shape[1]
    for b in range(own_width // LANES):
        first = pl.multiple_of(lax.axis_index("leaf") * own_width + b * LANES, LANES)
        own[:, b * LANES : (b + 1) * LANES] = values[pl.ds(first, LANES)].T[:classes]
    for write in writes:
        write.wait()


def finish(values, carried, ids):
    classes, rows = carried.shape
    own_width = values.shape[0] // lax.axis_size("leaf")
    return pl.pallas_call(
        finish_kernel,
        out_shape=(
            jax.ShapeDtypeStruct(carried.shape, F32),
            jax.ShapeDtypeStruct((classes, own_width), F32),
        ),
        in_specs=[
            pl.BlockSpec(memory_space=pltpu.VMEM),
            pl.BlockSpec(memory_space=pltpu.VMEM),
            pl.BlockSpec(memory_space=pl.ANY),
        ],
        out_specs=(pl.BlockSpec(memory_space=pl.ANY), pl.BlockSpec(memory_space=pltpu.VMEM)),
        scratch_shapes=[
            pltpu.VMEM((112, CHUNKS[-1] * LEAVES), BF16),
            pltpu.VMEM((CHUNKS[-1], rows), jnp.int32),
            pltpu.VMEM((classes, rows), F32),
            pltpu.SemaphoreType.DMA((WRITES,)),
            pltpu.SemaphoreType.DMA,
        ],
        compiler_params=pltpu.CompilerParams(vmem_limit_bytes=24 << 20),
        name="finish",
    )(values, carried, ids)


def shards(predict, labels, leaf_ids):
    carried, values = grow(predict, labels[None, :], leaf_ids)
    return finish(values, carried, leaf_ids)


def solution(mesh):
    finer = Mesh(mesh.devices.reshape(4, 4, 2, mesh.shape["leaf"]), AXES)
    in_specs = (P(None, AXES), P(AXES), P(None, AXES))
    out_specs = (P(None, AXES), P(None, "leaf"))
    return jax.shard_map(shards, mesh=finer, in_specs=in_specs, out_specs=out_specs, check_vma=False)
```
